256 devices in a mesh: dp: 32 (over x, y, core), expert: 8 (over z).
Axes of the slice: x: 4, y: 4, z: 8, core: 2. Of those that a mesh axis runs over, the one named last changes fastest.
Arguments:
- tokens: bfloat16 [1024, 4096], P('expert', 'dp'), may hold values from -6 to 6
- in_signs: int32 [1024, 128], P('expert', 'dp'), may hold values from -2147483648 to 2147483646
- out_signs: int32 [1024, 224], P('expert'), may hold values from -2147483648 to 2147483646
- expert_ids: int32 [1024, 2], P('expert'), may hold values from 0 to 7, all different within a row; in each aligned block of 128 rows (0 to 127, 128 to 255, ...) at most 40 rows name the same one
- route_weight: float32 [1024, 2], P('expert'), may hold values from 0.2 to 1
- cotangent: bfloat16 [1024, 7168], P('expert', 'dp'), may hold values from -6 to 6
- mean_weight: bfloat16 [8, 4096, 7168], P('expert', 'dp'), may hold values from -0.09375 to 0.09375
- rho_weight: bfloat16 [8, 4096, 7168], P('expert', 'dp'), may hold values from -6 to -3
- noise_weight: bfloat16 [8, 4096, 7168], P('expert', 'dp'), may hold values from -4 to 4
Outputs:
- hidden_out: bfloat16 [1024, 7168], P('expert', 'dp')
- grad_tokens: bfloat16 [1024, 4096], P('expert', 'dp')
- grad_mean: bfloat16 [8, 4096, 7168], P('expert', 'dp')
- grad_rho: bfloat16 [8, 4096, 7168], P('expert', 'dp')
The draws below stay inside these ranges and needn't reach their ends.
Inputs may be any that keep to these rules, and one draw needn't show every extreme that they name: `expert_ids`: each token names 2 different experts. In each aligned block of 128 tokens no expert is named by more than 40 tokens, and in some blocks one expert is named by exactly 40. `in_signs`: bit b of word w, counted from the lowest, is set where the sign of feature 32 * w + b is -1 and clear where it is +1. `out_signs`: bit b of word w, counted from the lowest, is set where the sign of hidden unit 32 * w + b is -1 and clear where it is +1.
All inputs are finite; a program needn't handle non-finite values.
Results may differ from the reference program's by a relative error of at most 0.0071.
Values may be sent and summed in bfloat16 or wider, within the bound.
A program may use at most 128 MiB of HBM per device.

```python
import math
import jax
import jax.numpy as jnp
import numpy as np
from jax import lax

D = 4096
FF = 7168
TOPK = 2
TOK_DEV = 128
EXPERTS = 8
CAP = 40
TOKENS = 1024
N_EXPERT = 8


def with_ends(array, stream_key, low, top_value):
    shape = array.shape
    index_at = [jax.random.randint(jax.random.fold_in(stream_key, axis), (), 0, shape[axis]) for axis in range(len(shape))]
    array = array.at[tuple(index_at)].set(low)
    longest = shape.index(max(shape))
    index_at[longest] = (index_at[longest] + 1) % shape[longest]
    return array.at[tuple(index_at)].set(top_value)


def block_scale(rng, extent, pieces, least, high):
    def one(axis_at, blocks):
        steps = jax.random.uniform(jax.random.fold_in(jax.random.fold_in(rng, 6), axis_at), (blocks,), jnp.float32, least / len(pieces), high / len(pieces))
        return jnp.repeat(jnp.exp(steps), extent[axis_at] // blocks).reshape((-1,) + (1,) * (len(extent) - axis_at - 1))

    loudness = one(*pieces[0])
    for cut in pieces[1:]:
        loudness = loudness * one(*cut)
    return loudness


def shared_out(key, own, number, rows, number_of, top, limit, skew):
    ranking = jax.random.permutation(key, number_of)
    heavy_load, common = shares(number_of, rows * top, limit, skew, True), shares(number_of, rows * top, limit, skew, False)
    places = jnp.arange(number_of)

    def named(sizes, turn):
        used = int((sizes > 0).sum())
        fixed = max(1, used // 4)
        moved = fixed + (places - fixed + turn * (used - fixed)) % max(1, number_of - fixed)
        return jnp.zeros((number_of,), jnp.int32).at[ranking[jnp.where(places < fixed, places, moved)]].set(jnp.asarray(sizes, jnp.int32))

    sizes = jnp.where(number % 4 == 0, named(heavy_load, number // 4), named(common, number - number // 4 - 1))
    mixed = jax.random.permutation(jax.random.fold_in(own, 3), number_of)
    giver, sink = mixed[0:number_of // 2 * 2:2], mixed[1:number_of // 2 * 2:2]
    slack = jnp.minimum(sizes[giver] - 1, limit - sizes[sink]) // 2
    slack = jnp.where((giver == ranking[0]) | (sink == ranking[0]) | (sizes[sink] == 0), 0, jnp.maximum(slack, 0))
    moved = jax.random.randint(jax.random.fold_in(own, 4), (number_of // 2,), 0, 1 << 20) % (slack + 1)
    sizes = sizes.at[giver].add(-moved).at[sink].add(moved)
    members = jnp.searchsorted(jnp.cumsum(sizes), jnp.arange(rows * top), side="right").astype(jnp.int32)
    listing = members.reshape(top, rows).T
    listing = listing[jax.random.permutation(jax.random.fold_in(own, 1), rows)]
    turn = jax.random.randint(jax.random.fold_in(own, 2), (rows, 1), 0, top)
    return jnp.take_along_axis(listing, (jnp.arange(top)[None, :] + turn) % top, axis=1)


def shares(count, total, limit, skew, full):
    weights = [(1 << 20) // math.isqrt(grade ** skew) + 1 for grade in range(1, count + 1)]
    largest = limit if full else min(limit, max(-(-total // count), total * weights[0] // sum(weights)))
    least = 1 if total - largest >= count - 1 else 0
    holding, surplus = [largest] + [least] * (count - 1), total - largest - least * (count - 1)
    while surplus > 0:
        free = [i for i in range(1, count) if holding[i] < largest] or [i for i in range(1, count) if holding[i] < limit]
        whole, remaining = sum([weights[i] for i in free]), surplus
        for i in free:
            more = min(limit - holding[i], max(1, remaining * weights[i] // whole), surplus)
            holding[i] = holding[i] + more
            surplus = surplus - more
    return np.array(holding)


def bell_draw(key, dims, deviation, most, cuts=(), kind=jnp.bfloat16):
    entries = jax.random.normal(key, dims, jnp.float32) * deviation
    if len(cuts) > 0:
        entries = block_scale(key, dims, cuts, -0.22, 0.18) * entries
    return jnp.clip(entries, min=-most, max=most).astype(kind)


def setup_inputs(seed: int = 0) -> dict:
    key_list = jax.random.split(jax.random.key(seed), 10)
    tokens = bell_draw(key_list[0], (TOKENS, D), 1.0, 6.0, ((0, 8), (1, 32)))
    in_signs = with_ends(jax.random.randint(key_list[1], (TOKENS, D // 32), -2147483648, 2147483647), jax.random.fold_in(key_list[1], 1), -2147483648, 2147483646).astype(jnp.int32)
    out_signs = with_ends(jax.random.randint(key_list[2], (TOKENS, FF // 32), -2147483648, 2147483647), jax.random.fold_in(key_list[2], 1), -2147483648, 2147483646).astype(jnp.int32)
    expert_ids_keys = jax.random.split(jax.random.fold_in(key_list[3], 1), TOKENS // TOK_DEV)
    expert_ids_turns = jax.random.permutation(jax.random.fold_in(key_list[3], 3), TOKENS // TOK_DEV)
    expert_ids = jax.vmap(lambda own, number: shared_out(jax.random.fold_in(key_list[3], 2), own, number, TOK_DEV, EXPERTS, TOPK, CAP, 2))(expert_ids_keys, expert_ids_turns).reshape((TOKENS, TOPK))
    route_weight = jnp.clip(0.2 + 0.8 * jax.random.uniform(key_list[4], (TOKENS, TOPK), jnp.float32) ** block_scale(key_list[4], (TOKENS, TOPK), ((0, 8),), -0.2, 0.2), 0.2, 1.0)
    cotangent = bell_draw(key_list[5], (TOKENS, FF), 1.0, 6.0, ((0, 8), (1, 32)))
    mean_weight = bell_draw(key_list[6], (EXPERTS, D, FF), D ** -0.5, 0.09375, ((0, 8), (1, 32)))
    rho_weight = jnp.clip(-6.0 + 3.0 * jax.random.uniform(key_list[7], (EXPERTS, D, FF), jnp.float32) ** block_scale(key_list[7], (EXPERTS, D, FF), ((0, 8), (1, 32)), -0.2, 0.2), -6.0, -3.0).astype(jnp.bfloat16)
    noise_weight = bell_draw(key_list[8], (EXPERTS, D, FF), 1.0, 4.0, ((0, 8), (1, 32)))
    return dict(tokens=tokens, in_signs=in_signs, out_signs=out_signs, expert_ids=expert_ids, route_weight=route_weight, cotangent=cotangent, mean_weight=mean_weight, rho_weight=rho_weight, noise_weight=noise_weight)


def unpack_rows(words):
    shifts = jnp.arange(32, dtype=jnp.int32)
    bits = jnp.bitwise_and(jnp.right_shift(words[..., None], shifts), 1)
    signs = (1 - 2 * bits).astype(jnp.float32)
    return signs.reshape(words.shape[:-1] + (words.shape[-1] * 32,))


def block_slots(block_ids):
    onehot = (block_ids[:, :, None] == jnp.arange(EXPERTS, dtype=jnp.int32)).astype(jnp.int32)
    flat = onehot.reshape(-1, EXPERTS)
    before = (jnp.cumsum(flat, axis=0) - flat).astype(jnp.int32)
    return jnp.sum(before * flat, axis=1).astype(jnp.int32).reshape(block_ids.shape)


def reference(tokens, in_signs, out_signs, expert_ids, route_weight, cotangent, mean_weight, rho_weight, noise_weight):
    blocks = expert_ids.reshape(N_EXPERT, TOK_DEV, TOPK)
    ranks = jax.vmap(block_slots)(blocks)
    source = jnp.arange(N_EXPERT, dtype=jnp.int32)[:, None, None]
    per_expert = N_EXPERT * CAP
    position = (blocks * per_expert + source * CAP + ranks).astype(jnp.int32).reshape(TOKENS, TOPK)
    total = EXPERTS * per_expert
    token_index = jnp.broadcast_to(jnp.arange(TOKENS, dtype=jnp.int32)[:, None], (TOKENS, TOPK))
    flat_pos = position.reshape(-1)
    slot_token = jnp.zeros((total,), jnp.int32).at[flat_pos].set(token_index.reshape(-1))
    slot_fill = jnp.zeros((total,), jnp.float32).at[flat_pos].set(1.0)
    slot_weight = jnp.zeros((total,), jnp.float32).at[flat_pos].set(route_weight.reshape(-1))
    input_full = unpack_rows(in_signs)
    output_full = unpack_rows(out_signs)

    def one_expert(operands):
        mean_e, rho_e, noise_e, tok_e, fill_e, weight_e = operands
        rows = jnp.take(tokens, tok_e, axis=0) * fill_e[:, None].astype(jnp.bfloat16)
        input_rows = jnp.take(input_full, tok_e, axis=0)
        output_rows = jnp.take(output_full, tok_e, axis=0)
        signed = rows * input_rows.astype(jnp.bfloat16)
        rho_float = rho_e.astype(jnp.float32)
        noise_float = noise_e.astype(jnp.float32)
        delta = (jax.nn.softplus(rho_float) * noise_float).astype(jnp.bfloat16)
        mean_part = jnp.dot(rows, mean_e, preferred_element_type=jnp.float32)
        pert_part = jnp.dot(signed, delta, preferred_element_type=jnp.float32)
        preact = mean_part + output_rows * pert_part
        gate = jax.nn.sigmoid(preact)
        hidden = (preact * gate).astype(jnp.bfloat16)
        upstream = (jnp.take(cotangent, tok_e, axis=0).astype(jnp.float32) * weight_e[:, None]).astype(jnp.bfloat16)
        slope = gate * (1.0 + preact * (1.0 - gate))
        grad_preact = (upstream.astype(jnp.float32) * slope).astype(jnp.bfloat16)
        grad_signed_pre = grad_preact * output_rows.astype(jnp.bfloat16)
        grad_mean_e = jnp.dot(rows.T, grad_preact, preferred_element_type=jnp.float32).astype(jnp.bfloat16)
        grad_delta = jnp.dot(signed.T, grad_signed_pre, preferred_element_type=jnp.float32)
        grad_rho_e = (grad_delta * noise_float * jax.nn.sigmoid(rho_float)).astype(jnp.bfloat16)
        back = jnp.dot(grad_preact, mean_e.T, preferred_element_type=jnp.float32)
        back = back + input_rows * jnp.dot(grad_signed_pre, delta.T, preferred_element_type=jnp.float32)
        return hidden, back.astype(jnp.bfloat16), grad_mean_e, grad_rho_e

    operands = (mean_weight, rho_weight, noise_weight, slot_token.reshape(EXPERTS, per_expert),
                slot_fill.reshape(EXPERTS, per_expert), slot_weight.reshape(EXPERTS, per_expert))
    hidden_slots, back_slots, grad_mean, grad_rho = lax.map(one_expert, operands)
    picked = jnp.take(hidden_slots.reshape(total, FF), position, axis=0).astype(jnp.float32)
    hidden_out = jnp.sum(picked * route_weight[:, :, None], axis=1).astype(jnp.bfloat16)
    returned = jnp.take(back_slots.reshape(total, D), position, axis=0).astype(jnp.float32)
    grad_tokens = jnp.sum(returned, axis=1).astype(jnp.bfloat16)
    return hidden_out, grad_tokens, grad_mean, grad_rho
```

```python
import jax
import jax.numpy as jnp
from jax import lax
from jax.sharding import PartitionSpec as P

F32 = jnp.float32
BF16 = jnp.bfloat16
NT = (((1,), (1,)), ((), ()))
TN = (((0,), (0,)), ((), ()))


def dot(a, b, dims=(((1,), (0,)), ((), ()))):
    return lax.dot_general(a, b, dims, preferred_element_type=F32)


def unpack_rows(words):
    shifts = jnp.arange(32, dtype=jnp.int32)
    bits = jnp.bitwise_and(jnp.right_shift(words[..., None], shifts), 1)
    return (1 - 2 * bits).astype(F32).reshape(words.shape[:-1] + (words.shape[-1] * 32,))


def bytes_of(words):
    parts = [jnp.bitwise_and(jnp.right_shift(words, 8 * j), 255) for j in range(4)]
    return jnp.concatenate(parts, axis=1).astype(F32).astype(BF16)


def words_of(parts):
    n = parts.shape[1] // 4
    out = parts[:, :n].astype(jnp.int32)
    for j in range(1, 4):
        out = out | (parts[:, j * n:(j + 1) * n].astype(jnp.int32) << (8 * j))
    return out


def on_device(tokens, in_signs, out_signs, expert_ids, route_weight, cotangent,
              mean_weight, rho_weight, noise_weight):
    experts = lax.axis_size("expert")
    token_count, width = tokens.shape
    topk = expert_ids.shape[1]
    capacity = 5 * token_count * topk // (4 * experts)
    slots = experts * capacity
    hidden_local = cotangent.shape[1]
    in_words = in_signs.shape[1]

    flat_ids = expert_ids.reshape(-1)
    pairs = token_count * topk
    onehot = (flat_ids[:, None] == jnp.arange(experts, dtype=jnp.int32)).astype(BF16)
    lower = (jnp.arange(pairs)[:, None] > jnp.arange(pairs)[None, :]).astype(BF16)
    before = dot(lower, onehot)
    ranks = jnp.sum(before * onehot.astype(F32), axis=1).astype(jnp.int32)
    slot_of = (flat_ids * capacity + ranks).reshape(token_count, topk)
    slot_ids = jnp.arange(slots, dtype=jnp.int32)
    picks = [slot_of[:, k][:, None] == slot_ids[None, :] for k in range(topk)]
    pick = [p.astype(BF16) for p in picks]
    gather = sum(pick[1:], pick[0])
    slot_weight = sum(
        jnp.sum(jnp.where(p, route_weight[:, k][:, None], 0.0), axis=0)
        for k, p in enumerate(picks)
    )

    words = jnp.concatenate([in_signs, out_signs], axis=1)
    send_rows = dot(gather, tokens, TN).astype(BF16)
    send_cot = dot(gather, cotangent, TN) * slot_weight[:, None]
    send_words = words_of(dot(gather, bytes_of(words), TN))
    send = jnp.concatenate([send_rows, send_cot.astype(BF16)], axis=1)
    recv = lax.all_to_all(send.reshape(experts, capacity, -1), "expert", 0, 0, tiled=True)
    recv_words = lax.all_to_all(
        send_words.reshape(experts, capacity, -1), "expert", 0, 0, tiled=True)
    recv = recv.reshape(slots, -1)
    recv_words = recv_words.reshape(slots, -1)
    rows = recv[:, :width]
    upstream = recv[:, width:].T
    in_s = unpack_rows(recv_words[:, :in_words])
    signed = rows * in_s.astype(BF16)
    wt = recv_words[:, in_words:].T
    bit = (wt[:, None, :] >> jnp.arange(32, dtype=jnp.int32)[None, :, None]) & 1
    flip = bit.reshape(-1, slots)
    r_all = (1 - 2 * flip).astype(BF16)

    mean = mean_weight[0]
    rho = rho_weight[0].astype(F32)
    noise = noise_weight[0].astype(F32)
    delta = (jax.nn.softplus(rho) * noise).astype(BF16)
    part = dot(mean, rows, (((0,), (1,)), ((), ())))
    pert = dot(delta, signed, (((0,), (1,)), ((), ())))
    part = (part + pert * r_all.astype(F32)).astype(BF16)
    preact = lax.psum_scatter(part, "dp", scatter_dimension=0, tiled=True).astype(F32)
    gate = jax.nn.sigmoid(preact)
    hidden = (preact * gate).astype(BF16)
    slope = gate * (1.0 + preact * (1.0 - gate))
    dy_local = (upstream.astype(F32) * slope).astype(BF16)
    hid = lax.all_to_all(hidden.T.reshape(experts, capacity, -1), "expert", 0, 0, tiled=True)
    hid = hid.reshape(slots, -1)
    hidden_out = sum(
        dot(pick[k], hid) * route_weight[:, k][:, None] for k in range(topk)
    ).astype(BF16)

    dy = lax.all_gather(dy_local, "dp", axis=0, tiled=True)
    dyr = dy * r_all
    back = dot(mean, dy) + in_s.T * dot(delta, dyr)
    back = back.T.astype(BF16)
    ret = lax.all_to_all(back.reshape(experts, capacity, -1), "expert", 0, 0, tiled=True)
    grad_tokens = dot(gather, ret.reshape(slots, -1)).astype(BF16)
    grad_mean = dot(rows, dy, (((0,), (1,)), ((), ()))).astype(BF16)[None]
    gdelta = dot(signed, dyr, (((0,), (1,)), ((), ())))
    grad_rho = (gdelta * noise * jax.nn.sigmoid(rho)).astype(BF16)[None]
    return hidden_out, grad_tokens, grad_mean, grad_rho


def solution(mesh):
    row = P("expert", "dp")
    full = P("expert", None)
    weight = P("expert", "dp", None)
    return jax.shard_map(
        on_device, mesh=mesh,
        in_specs=(row, row, full, full, full, row, weight, weight, weight),
        out_specs=(row, row, weight, weight), check_vma=False)
```

```python
import functools

import jax
import jax.numpy as jnp
from jax import lax
from jax.experimental import pallas as pl
from jax.experimental.pallas import tpu as pltpu
from jax.sharding import PartitionSpec as P

F32 = jnp.float32
BF16 = jnp.bfloat16
I32 = jnp.int32
MESH = pl.DeviceIdType.MESH
NN = (((1,), (0,)), ((), ()))
TN = (((0,), (0,)), ((), ()))
VMEM = pl.BlockSpec(memory_space=pltpu.VMEM)

SIDE = 4
HALF = 112
OFFS = (2, 1, 3, 0)
CUT = ((0, 64), (64, 48))


def dot(a, b, dims=NN):
    return lax.dot_general(a, b, dims, preferred_element_type=F32)


def prep_kernel(mean_ref, rho_ref, noise_ref, wm_ref, wd_ref, vm_ref, vd_ref):
    delta = (jax.nn.softplus(rho_ref[...].astype(F32)) * noise_ref[...].astype(F32)).astype(BF16)
    for src, wt, w3 in ((mean_ref[...], wm_ref, vm_ref), (delta, wd_ref, vd_ref)):
        t = src.T
        for d in range(4):
            for h in range(2):
                at = (2 * d + h) * HALF
                wt[0, d * HALF:(d + 1) * HALF, h * 128:(h + 1) * 128] = t[at:at + HALF]
        w3[0] = wt[0].T


def prep(mean, rho, noise):
    blk = pl.BlockSpec((128, 896), lambda i: (0, i))
    tall = pl.BlockSpec((1, 448, 256), lambda i: (i, 0, 0))
    wide = pl.BlockSpec((1, 256, 448), lambda i: (i, 0, 0))
    return pl.pallas_call(
        prep_kernel,
        grid=(8,),
        in_specs=[blk, blk, blk],
        out_specs=[tall, tall, wide, wide],
        out_shape=[jax.ShapeDtypeStruct((8, 448, 256), BF16)] * 2
        + [jax.ShapeDtypeStruct((8, 256, 448), BF16)] * 2,
        cost_estimate=pl.CostEstimate(flops=40_000_000, bytes_accessed=13_000_000, transcendentals=2_000_000),
        name="weights",
    )(mean, rho, noise)


def swap_kernel(n, *refs):
    ins, outs, (send, recv) = refs[:n], refs[n:2 * n], refs[2 * n:]
    me = lax.axis_index("expert")
    barrier = pltpu.get_barrier_semaphore()
    for o in range(1, 8):
        pl.semaphore_signal(barrier, inc=1, device_id={"expert": lax.rem(me + o, 8)}, device_id_type=MESH)
    pl.semaphore_wait(barrier, 7)
    copies = []
    for i in range(n):
        for o in (4, 3, 5, 2, 6, 1, 7):
            to = lax.rem(me + o, 8)
            c = pltpu.make_async_remote_copy(
                ins[i].at[to], outs[i].at[me], send.at[i * 7 + o - 1], recv.at[i * 7 + o - 1],
                device_id={"expert": to}, device_id_type=MESH)
            c.start()
            copies.append(c)
    for i in range(n):
        outs[i][me] = ins[i][me]
    for c in copies:
        c.wait_recv()
    for c in copies:
        c.wait_send()


def swap(arrays, cid):
    n = len(arrays)
    return pl.pallas_call(
        functools.partial(swap_kernel, n),
        in_specs=[VMEM] * n,
        out_specs=[VMEM] * n,
        out_shape=[jax.ShapeDtypeStruct(a.shape, a.dtype) for a in arrays],
        scratch_shapes=[pltpu.SemaphoreType.DMA((7 * n,)), pltpu.SemaphoreType.DMA((7 * n,))],
        compiler_params=pltpu.CompilerParams(collective_id=cid, has_side_effects=True),
        name=f"swap{cid}",
    )(*arrays)


def sign_rows(l_ref, d, j):
    i = j // 2
    lane = lax.broadcasted_iota(I32, (1, 640), 1)
    if j % 2 == 0:
        row = jnp.where(lane < 320, l_ref[d, i:i + 1], l_ref[d, i:i + 1] >> 16)
    else:
        row = jnp.where(lane < 320, l_ref[d, i:i + 1] >> 16, l_ref[d, i + 1:i + 2])
    return (jnp.broadcast_to(row, (16, 640)) >> lax.broadcasted_iota(I32, (16, 640), 0)) & 1


def forward_kernel(wm_ref, wd_ref, l_ref, a_ref, b_ref, p_ref, m_ref, d_ref):
    m_ref[...] = dot(wm_ref[0], a_ref[...])
    d_ref[...] = dot(wd_ref[0], b_ref[...])
    for d in range(4):
        for j in range(7):
            at = d * HALF + 16 * j
            pert = d_ref[at:at + 16]
            pert = jnp.where(sign_rows(l_ref, d, j) != 0, -pert, pert)
            p_ref[d, 16 * j:16 * j + 16] = (m_ref[at:at + 16] + pert).astype(BF16)


def forward(wm, wd, lanes, a2, b2):
    tall = pl.BlockSpec((1, 448, 256), lambda i: (i, 0, 0))
    fixed = pl.BlockSpec((256, 640), lambda i: (0, 0))
    return pl.pallas_call(
        forward_kernel,
        grid=(8,),
        in_specs=[tall, tall, pl.BlockSpec((4, 4, 640), lambda i: (i, 0, 0)), fixed, fixed],
        out_specs=pl.BlockSpec((4, HALF, 640), lambda i: (i, 0, 0)),
        out_shape=jax.ShapeDtypeStruct((32, HALF, 640), BF16),
        scratch_shapes=[pltpu.VMEM((448, 640), F32), pltpu.VMEM((448, 640), F32)],
        name="products",
    )(wm, wd, lanes, a2, b2)


def ring_kernel(p_ref, up_ref, d_ref, h_ref, r0, q, t1, rp, rm, s, t2, rp2, rm2, send, recv):
    me = lax.axis_index("dp")
    k = lax.rem(me, 2)
    x, y = me // 8, lax.rem(me // 2, SIDE)
    a, b = x * (1 - k) + y * k, y * (1 - k) + x * k
    sa, sb = 8 - 6 * k, 2 + 6 * k
    partner = me + 1 - 2 * k

    def at(da, db):
        return lax.rem(a + da, SIDE) * sa + lax.rem(b + db, SIDE) * sb + k

    up_a, down_a, up_b, down_b = at(1, 0), at(3, 0), at(0, 1), at(0, 3)
    barrier = pltpu.get_barrier_semaphore()
    for peer in (partner, up_a, down_a, up_b, down_b):
        pl.semaphore_signal(barrier, inc=1, device_id={"dp": peer}, device_id_type=MESH)
    pl.semaphore_wait(barrier, 5)

    copies = []

    def put(src, dst, to):
        i = len(copies)
        c = pltpu.make_async_remote_copy(
            src, dst, send.at[i], recv.at[i], device_id={"dp": to}, device_id_type=MESH)
        c.start()
        copies.append(c)
        return c

    pair = {}
    for g in range(4):
        for r in range(4):
            theirs = (lax.rem(b + OFFS[g], SIDE) * sb + lax.rem(a + OFFS[r], SIDE) * sa + (1 - k))
            pair[g, r] = put(p_ref.at[theirs], r0.at[4 * g + r], partner)

    def merge(g, r):
        pair[g, r].wait_recv()
        q[4 * g + r] = p_ref[at(OFFS[g], OFFS[r])] + r0[4 * g + r]

    def qq(g, r):
        return q.at[4 * g + r]

    far, plus, minus = {}, {}, {}
    for r in (0, 1, 2, 3):
        merge(0, r)
        far[r] = put(qq(0, r), t1.at[r], up_a if r in (0, 3) else down_a)
    merge(2, 0)
    minus[0] = put(qq(2, 0), rm.at[0], down_a)
    merge(1, 0)
    merge(1, 1)
    merge(2, 1)

    def relay(r):
        far[r].wait_recv()
        g = 1 if r in (0, 3) else 2
        q[4 * g + r] = q[4 * g + r] + t1[r]
        if g == 1:
            plus[r] = put(qq(1, r), rp.at[r], up_a)
        else:
            minus[r] = put(qq(2, r), rm.at[r], down_a)

    relay(0)
    plus[1] = put(qq(1, 1), rp.at[1], up_a)
    relay(1)
    merge(1, 2)
    plus[2] = put(qq(1, 2), rp.at[2], up_a)
    merge(2, 2)
    relay(2)
    merge(2, 3)
    minus[3] = put(qq(2, 3), rm.at[3], down_a)
    merge(1, 3)
    relay(3)
    for r in range(4):
        merge(3, r)

    def total(r):
        plus[r].wait_recv()
        minus[r].wait_recv()
        return q[12 + r].astype(F32) + rp[r].astype(F32) + rm[r].astype(F32)

    (o0, n0), (o1, n1) = CUT
    c0, c1 = pl.ds(o0, n0), pl.ds(o1, n1)
    s[0] = total(0).astype(BF16)
    far_up = put(s.at[0, c0], t2.at[c0], up_b)
    far_dn = put(s.at[0, c1], t2.at[c1], down_b)
    s[1] = total(1).astype(BF16)
    p1 = put(s.at[1, c1], rp2.at[c1], up_b)
    s[2] = total(2).astype(BF16)
    m1 = put(s.at[2, c0], rm2.at[c0], down_b)
    far_up.wait_recv()
    s[1, c0] = s[1, c0] + t2[c0]
    p2 = put(s.at[1, c0], rp2.at[c0], up_b)
    far_dn.wait_recv()
    s[2, c1] = s[2, c1] + t2[c1]
    m2 = put(s.at[2, c1], rm2.at[c1], down_b)
    own = total(3)
    for c in (p1, m1, p2, m2):
        c.wait_recv()
    pre = own + rp2[...].astype(F32) + rm2[...].astype(F32)
    gate = jax.nn.sigmoid(pre)
    h_ref[...] = (pre * gate).astype(BF16)
    slope = gate * (1.0 + pre * (1.0 - gate))
    d_ref[me] = (up_ref[...].astype(F32) * slope).astype(BF16)

    def hand(da, db):
        i = at(da, db)
        return put(d_ref.at[i], d_ref.at[i], partner)

    def spread(db):
        i = at(0, db)
        up = put(d_ref.at[i], d_ref.at[i], up_a)
        dn = put(d_ref.at[i], d_ref.at[i], down_a)
        hand(0, db)
        return up, dn

    b_up = put(d_ref.at[me], d_ref.at[me], up_b)
    b_dn = put(d_ref.at[me], d_ref.at[me], down_b)
    sent = {0: spread(0)}
    b_up.wait_recv()
    i = at(0, 3)
    f_up = put(d_ref.at[i, c0], d_ref.at[i, c0], up_b)
    b_dn.wait_recv()
    i = at(0, 1)
    f_dn = put(d_ref.at[i, c1], d_ref.at[i, c1], down_b)
    sent[3] = spread(3)
    sent[1] = spread(1)

    fwd = {}

    def arrive(db):
        up, dn = sent[db]
        up.wait_recv()
        if db in (0, 2):
            i = at(3, db)
            fwd[db] = put(d_ref.at[i], d_ref.at[i], up_a)
        hand(3, db)
        dn.wait_recv()
        if db in (1, 3):
            i = at(1, db)
            fwd[db] = put(d_ref.at[i], d_ref.at[i], down_a)
        hand(1, db)

    arrive(0)
    f_up.wait_recv()
    f_dn.wait_recv()
    sent[2] = spread(2)
    arrive(3)
    arrive(1)
    arrive(2)
    for db in (0, 3, 1, 2):
        fwd[db].wait_recv()
        hand(2, db)
    waited = set(map(id, list(pair.values()) + list(far.values()) + list(plus.values()) + list(minus.values())
                     + [far_up, far_dn, p1, m1, p2, m2, b_up, b_dn, f_up, f_dn] + list(fwd.values())
                     + [c for two in sent.values() for c in two]))
    for c in copies:
        if id(c) not in waited:
            c.wait_recv()
    for c in copies:
        c.wait_send()


COPIES = 16 + 12 + 6 + 2 + 2 + 8 + 4 + 16


def ring(part, up):
    blk = lambda n: pltpu.VMEM((n, HALF, 640), BF16)
    one = pltpu.VMEM((HALF, 640), BF16)
    return pl.pallas_call(
        ring_kernel,
        in_specs=[VMEM, VMEM],
        out_specs=[VMEM, VMEM],
        out_shape=[jax.ShapeDtypeStruct((32, HALF, 640), BF16), jax.ShapeDtypeStruct((HALF, 640), BF16)],
        scratch_shapes=[blk(16), blk(16), blk(4), blk(4), blk(4), blk(3), one, one, one,
                        pltpu.SemaphoreType.DMA((COPIES,)), pltpu.SemaphoreType.DMA((COPIES,))],
        compiler_params=pltpu.CompilerParams(
            collective_id=1, has_side_effects=True, vmem_limit_bytes=56 * 1024 * 1024),
        name="ring",
    )(part, up)


def backward_kernel(dy_ref, l_ref, a_ref, b_ref, vm_ref, vd_ref, rho_ref, noise_ref, s_ref,
                    gm_ref, gr_ref, g_ref, dyr, accm, accd):
    step = pl.program_id(0)

    @pl.when(step == 0)
    def _():
        accm[...] = jnp.zeros_like(accm)
        accd[...] = jnp.zeros_like(accd)

    for d in range(4):
        for j in range(7):
            at = d * HALF + 16 * j
            v = dy_ref[d, 16 * j:16 * j + 16].astype(F32)
            dyr[at:at + 16] = jnp.where(sign_rows(l_ref, d, j) != 0, -v, v).astype(BF16)
    dy = dy_ref[...].reshape(448, 640)
    accm[...] += dot(vm_ref[0], dy)
    accd[...] += dot(vd_ref[0], dyr[...])

    def unfold(g):
        return jnp.concatenate(
            [g[d * HALF:(d + 1) * HALF, h * 128:(h + 1) * 128] for d in range(4) for h in range(2)], axis=0)

    gm_ref[...] = unfold(dot(dy, a_ref[...])).T.astype(BF16)
    gd = unfold(dot(dyr[...], b_ref[...])).T
    gr_ref[...] = (gd * noise_ref[...].astype(F32) * jax.nn.sigmoid(rho_ref[...].astype(F32))).astype(BF16)

    @pl.when(step == 7)
    def _():
        plain = accm[0:128, 0:320] + accm[128:256, 320:640]
        pert = accd[0:128, 0:320] + accd[128:256, 320:640]
        g = (plain + s_ref[...] * pert).T
        for e in range(8):
            g_ref[e] = g[40 * e:40 * e + 40].astype(BF16)


def backward(dy, lanes, a3, b3, vm, vd, rho, noise, s_cols):
    blk = pl.BlockSpec((128, 896), lambda i: (0, i))
    wide = pl.BlockSpec((1, 256, 448), lambda i: (i, 0, 0))
    fixed = pl.BlockSpec((640, 256), lambda i: (0, 0))
    return pl.pallas_call(
        backward_kernel,
        grid=(8,),
        in_specs=[pl.BlockSpec((4, HALF, 640), lambda i: (i, 0, 0)),
                  pl.BlockSpec((4, 4, 640), lambda i: (i, 0, 0)), fixed, fixed, wide, wide, blk, blk,
                  pl.BlockSpec((128, 320), lambda i: (0, 0))],
        out_specs=[blk, blk, pl.BlockSpec((8, 40, 128), lambda i: (0, 0, 0))],
        out_shape=[jax.ShapeDtypeStruct((128, 7168), BF16)] * 2 + [jax.ShapeDtypeStruct((8, 40, 128), BF16)],
        scratch_shapes=[pltpu.VMEM((448, 640), BF16), pltpu.VMEM((256, 640), F32), pltpu.VMEM((256, 640), F32)],
        name="gradients",
    )(dy, lanes, a3, b3, vm, vd, rho, noise, s_cols)


def unpack_rows(words):
    bits = (words[..., None] >> jnp.arange(32, dtype=I32)) & 1
    return (1 - 2 * bits).astype(F32).reshape(words.shape[:-1] + (words.shape[-1] * 32,))


def bytes_of(words):
    parts = [(words >> (8 * j)) & 255 for j in range(4)]
    return jnp.concatenate(parts, axis=1).astype(F32).astype(BF16)


def words_of(parts):
    n = parts.shape[1] // 4
    ints = parts.astype(I32)
    return ints[:, :n] | (ints[:, n:2 * n] << 8) | (ints[:, 2 * n:3 * n] << 16) | (ints[:, 3 * n:] << 24)


def doubled(m):
    zero = jnp.zeros_like(m)
    return jnp.concatenate(
        [jnp.concatenate([m, zero], axis=1), jnp.concatenate([zero, m], axis=1)], axis=0)


def on_device(tokens, in_signs, out_signs, expert_ids, route_weight, cotangent,
              mean_weight, rho_weight, noise_weight):
    experts, capacity, slots, topk = 8, 40, 320, 2
    token_count = tokens.shape[0]

    wm, wd, vm, vd = prep(mean_weight[0], rho_weight[0], noise_weight[0])

    flat_ids = expert_ids.reshape(-1)
    pairs = token_count * topk
    onehot = (flat_ids[:, None] == jnp.arange(experts, dtype=I32)).astype(BF16)
    lower = (jnp.arange(pairs)[:, None] > jnp.arange(pairs)[None, :]).astype(BF16)
    before = dot(lower, onehot)
    ranks = jnp.sum(before * onehot.astype(F32), axis=1).astype(I32)
    slot_of = (flat_ids * capacity + ranks).reshape(token_count, topk)
    slot_ids = jnp.arange(slots, dtype=I32)
    picks = [slot_of[:, k][:, None] == slot_ids[None, :] for k in range(topk)]
    pick = [p.astype(BF16) for p in picks]
    gather = pick[0] + pick[1]
    slot_weight = sum(
        jnp.sum(jnp.where(p, route_weight[:, k][:, None], 0.0), axis=0) for k, p in enumerate(picks))

    send_rows = dot(gather, tokens, TN).astype(BF16)
    send_cot = (dot(gather, cotangent, TN) * slot_weight[:, None]).astype(BF16)
    send_words = words_of(dot(gather, bytes_of(jnp.concatenate([out_signs, in_signs], axis=1)), TN))
    rows, words, up = swap(
        [v.reshape(experts, capacity, -1) for v in (send_rows, send_words, send_cot)], 2)
    rows, words, up = (v.reshape(slots, -1) for v in (rows, words, up))

    in_s = unpack_rows(words[:, 224:])
    signed = rows * in_s.astype(BF16)
    wt = words[:, :224].T.reshape(32, 7, slots)
    lanes = jnp.concatenate([wt[:, 0:4], wt[:, 3:7]], axis=2)
    up2 = up.T
    up2 = jnp.concatenate([up2[:HALF], up2[HALF:]], axis=1)

    part = forward(wm, wd, lanes, doubled(rows.T), doubled(signed.T))
    dy, hid = ring(part, up2)
    grad_mean, grad_rho, g = backward(
        dy, lanes, doubled(rows), doubled(signed), vm, vd, rho_weight[0], noise_weight[0], in_s.T)
    hid = jnp.concatenate([hid[:, :slots], hid[:, slots:]], axis=0).T
    hid, back = swap([hid.reshape(experts, capacity, -1), g], 3)
    hid = hid.reshape(slots, -1)
    hidden_out = (dot(pick[0], hid) * route_weight[:, 0:1]
                  + dot(pick[1], hid) * route_weight[:, 1:2]).astype(BF16)
    grad_tokens = dot(gather, back.reshape(slots, -1)).astype(BF16)
    return hidden_out, grad_tokens, grad_mean[None], grad_rho[None]


def solution(mesh):
    row = P("expert", "dp")
    full = P("expert", None)
    weight = P("expert", "dp", None)
    return jax.shard_map(
        on_device, mesh=mesh,
        in_specs=(row, row, full, full, full, row, weight, weight, weight),
        out_specs=(row, row, weight, weight), check_vma=False)
```

```python
import jax
import jax.numpy as jnp
from jax import lax
from jax.experimental import pallas as pl
from jax.experimental.pallas import tpu as pltpu
from jax.sharding import PartitionSpec as P

F32 = jnp.float32
BF16 = jnp.bfloat16
I32 = jnp.int32
MESH = pl.DeviceIdType.MESH
NN = (((1,), (0,)), ((), ()))
TN = (((0,), (0,)), ((), ()))
VMEM = pl.BlockSpec(memory_space=pltpu.VMEM)

SIDE = 4
HALF = 112
OFFS = (2, 1, 3, 0)
CUT = ((0, 64), (64, 48))


def dot(a, b, dims=NN):
    return lax.dot_general(a, b, dims, preferred_element_type=F32)


ZORDER = (4, 3, 5, 2, 6, 1, 7)
UNITS = 7168
BLOCK = 896
COPIES = 35 + 1 + 16 + 12 + 6 + 2 + 2 + 8 + 4 + 16


def layer_kernel(rows_in, words_in, cot_in, mean_hbm, rho_hbm, noise_hbm,
                 hid_out, back_out, gm_hbm, gr_hbm,
                 mean, rho, noise, wm, wd, rows_r, words_r, words_p, cot_r, w2, bda, bdb, ba, bb, sgn_t,
                 up2, mx, dx, p, r0, q, t1, rp, rm, s, t2, rp2, rm2, dbuf, hs, dyr, accm, accd,
                 gt, gdt, gs, gm, gr, send, recv, local):
    me, z = lax.axis_index("dp"), lax.axis_index("expert")
    k = lax.rem(me, 2)
    x, y = me // 8, lax.rem(me // 2, SIDE)
    a, b = x * (1 - k) + y * k, y * (1 - k) + x * k
    sa, sb = 8 - 6 * k, 2 + 6 * k
    partner = me + 1 - 2 * k

    def at(da, db):
        return lax.rem(a + da, SIDE) * sa + lax.rem(b + db, SIDE) * sb + k

    def theirs(db, da):
        return lax.rem(b + db, SIDE) * sb + lax.rem(a + da, SIDE) * sa + (1 - k)

    up_a, down_a, up_b, down_b = at(1, 0), at(3, 0), at(0, 1), at(0, 3)

    loads = [pltpu.make_async_copy(src, dst, local.at[16 + i]) for i, (src, dst) in enumerate(
        ((rho_hbm, rho), (noise_hbm, noise), (mean_hbm, mean)))]
    for c in loads:
        c.start()
    barrier = pltpu.get_barrier_semaphore()
    for o in ZORDER:
        pl.semaphore_signal(barrier, inc=1, device_id={"expert": lax.rem(z + o, 8)}, device_id_type=MESH)
    for peer in (up_a, down_a, up_b, down_b, partner):
        pl.semaphore_signal(barrier, inc=1, device_id={"dp": peer}, device_id_type=MESH)
    pl.semaphore_wait(barrier, 12)

    copies, done = [], set()

    def put(src, dst, to, axis="dp"):
        i = len(copies)
        c = pltpu.make_async_remote_copy(
            src, dst, send.at[i], recv.at[i], device_id={axis: to}, device_id_type=MESH)
        c.start()
        copies.append(c)
        return c

    def arrived(c):
        done.add(id(c))
        c.wait_recv()

    def swap(src, dst):
        out = []
        for o in ZORDER:
            to = lax.rem(z + o, 8)
            out.append(put(src.at[to], dst.at[z], to, "expert"))
        return out

    z_words = swap(words_in, words_r)
    z_rows = swap(rows_in, rows_r)
    z_cot = swap(cot_in, cot_r)
    words_r[z] = words_in[z]
    rows_r[z] = rows_in[z]
    cot_r[z] = cot_in[z]

    for c in loads:
        c.wait()

    def fold(i, carry):
        cols = pl.ds(pl.multiple_of(i * BLOCK, 128), BLOCK)
        delta = (jax.nn.softplus(rho[:, cols].astype(F32)) * noise[:, cols].astype(F32)).astype(BF16)
        for v, wt in ((mean[:, cols], wm), (delta, wd)):
            t = v.T
            for d in range(4):
                for h in range(2):
                    o = (2 * d + h) * HALF
                    wt[4 * i + d, :, h * 128:(h + 1) * 128] = t[o:o + HALF]
        return carry

    lax.fori_loop(0, 8, fold, 0)

    def slots_of(ref):
        return jnp.concatenate([ref[e].astype(F32) for e in range(8)], axis=0)

    for c in z_words:
        arrived(c)
    pair_words = put(words_r, words_p, partner)
    words = jnp.concatenate([words_r[e] for e in range(8)], axis=0)
    wt = words.T
    w2[k] = jnp.concatenate([wt, wt], axis=1)
    lane = lax.broadcasted_iota(I32, (320, 128), 1)
    word = jnp.broadcast_to(words[:, 115:116], (320, 128))
    for w in range(3):
        word = jnp.where(lane // 32 == w, jnp.broadcast_to(words[:, 112 + w:113 + w], (320, 128)), word)
    sgn = (1 - 2 * ((word >> (lane & 31)) & 1)).astype(F32)
    for c in z_rows:
        arrived(c)
    plain = slots_of(rows_r)
    signed = plain * sgn
    sgn_t[...] = sgn.T
    none_w, none_t = jnp.zeros((128, 320), F32), jnp.zeros((320, 128), F32)
    for v, wide, tall in ((plain, bda, ba), (signed, bdb, bb)):
        t = v.T
        wide[0:128] = jnp.concatenate([t, none_w], axis=1).astype(BF16)
        wide[128:256] = jnp.concatenate([none_w, t], axis=1).astype(BF16)
        tall[0:320] = jnp.concatenate([v, none_t], axis=1).astype(BF16)
        tall[320:640] = jnp.concatenate([none_t, v], axis=1).astype(BF16)
    arrived(pair_words)
    wt = jnp.concatenate([words_p[e] for e in range(8)], axis=0).T
    w2[1 - k] = jnp.concatenate([wt, wt], axis=1)

    left = lax.broadcasted_iota(I32, (1, 640), 1) < 320
    down16 = lax.broadcasted_iota(I32, (16, 640), 0)

    def minus_at(dd, j):
        half, base = dd // 16, lax.rem(dd, 16) * 7
        one = w2[half, pl.ds(base + j // 2, 1), :] >> (16 * (j % 2))
        two = w2[half, pl.ds(base + 3 + (j + 1) // 2, 1), :] >> (16 * ((j + 1) % 2))
        return ((jnp.broadcast_to(jnp.where(left, one, two), (16, 640)) >> down16) & 1) != 0

    def products(dd_of):
        mx[...] = dot(jnp.concatenate([wm[dd_of(r)] for r in range(4)], axis=0), bda[...])
        dx[...] = dot(jnp.concatenate([wd[dd_of(r)] for r in range(4)], axis=0), bdb[...])

        def combine(r, carry):
            dd = dd_of(r)
            for j in range(7):
                rows = pl.ds(pl.multiple_of(r * HALF + 16 * j, 16), 16)
                pert = dx[rows]
                p[dd, 16 * j:16 * j + 16] = (
                    mx[rows] + jnp.where(minus_at(dd, j), -pert, pert)).astype(BF16)
            return carry

        lax.fori_loop(0, 4, combine, 0)

    pair = {}

    def products_pair(g):
        products(lambda r: theirs(OFFS[g], r))
        for r in range(4):
            pair[g, r] = put(p.at[theirs(OFFS[g], OFFS[r])], r0.at[4 * g + r], partner)

    def products_own(g):
        products(lambda r: at(OFFS[g], r))

    def merge(g, r):
        arrived(pair[g, r])
        q[4 * g + r] = p[at(OFFS[g], OFFS[r])] + r0[4 * g + r]

    def qq(g, r):
        return q.at[4 * g + r]

    far, plus, minus = {}, {}, {}
    products_pair(0)
    products_own(0)
    products_pair(1)
    for r in range(4):
        merge(0, r)
        far[r] = put(qq(0, r), t1.at[r], up_a if r in (0, 3) else down_a)
    products_pair(2)
    products_own(1)
    products_own(2)

    def relay(r):
        arrived(far[r])
        g = 1 if r in (0, 3) else 2
        q[4 * g + r] = q[4 * g + r] + t1[r]
        if g == 1:
            plus[r] = put(qq(1, r), rp.at[r], up_a)
        else:
            minus[r] = put(qq(2, r), rm.at[r], down_a)

    merge(2, 0)
    minus[0] = put(qq(2, 0), rm.at[0], down_a)
    merge(1, 0)
    relay(0)
    merge(1, 1)
    plus[1] = put(qq(1, 1), rp.at[1], up_a)
    merge(2, 1)
    relay(1)
    merge(1, 2)
    plus[2] = put(qq(1, 2), rp.at[2], up_a)
    merge(2, 2)
    relay(2)
    merge(2, 3)
    minus[3] = put(qq(2, 3), rm.at[3], down_a)
    merge(1, 3)
    relay(3)
    products_pair(3)
    products_own(3)
    for c in z_cot:
        arrived(c)
    ut = slots_of(cot_r).T
    up2[...] = jnp.concatenate([ut[:HALF], ut[HALF:]], axis=1)
    for r in range(4):
        merge(3, r)

    def total(r):
        arrived(plus[r])
        arrived(minus[r])
        return q[12 + r].astype(F32) + rp[r].astype(F32) + rm[r].astype(F32)

    (o0, n0), (o1, n1) = CUT
    c0, c1 = pl.ds(o0, n0), pl.ds(o1, n1)
    s[0] = total(0).astype(BF16)
    far_up = put(s.at[0, c0], t2.at[c0], up_b)
    far_dn = put(s.at[0, c1], t2.at[c1], down_b)
    s[1] = total(1).astype(BF16)
    p1 = put(s.at[1, c1], rp2.at[c1], up_b)
    s[2] = total(2).astype(BF16)
    m1 = put(s.at[2, c0], rm2.at[c0], down_b)
    arrived(far_up)
    s[1, c0] = s[1, c0] + t2[c0]
    p2 = put(s.at[1, c0], rp2.at[c0], up_b)
    arrived(far_dn)
    s[2, c1] = s[2, c1] + t2[c1]
    m2 = put(s.at[2, c1], rm2.at[c1], down_b)
    own = total(3)
    for c in (p1, m1, p2, m2):
        arrived(c)

    pre = own + rp2[...].astype(F32) + rm2[...].astype(F32)
    gate = jax.nn.sigmoid(pre)
    slope = gate * (1.0 + pre * (1.0 - gate))
    dbuf[me] = (up2[...] * slope).astype(BF16)

    def hand(da, db):
        i = at(da, db)
        hands[da, db] = put(dbuf.at[i], dbuf.at[i], partner)

    def spread(db):
        i = at(0, db)
        up = put(dbuf.at[i], dbuf.at[i], up_a)
        dn = put(dbuf.at[i], dbuf.at[i], down_a)
        hand(0, db)
        return up, dn

    hands = {}
    b_up = put(dbuf.at[me], dbuf.at[me], up_b)
    b_dn = put(dbuf.at[me], dbuf.at[me], down_b)
    sent = {0: spread(0)}

    ht = (pre * gate).T
    for e in range(8):
        hs[e] = jnp.concatenate(
            [ht[40 * e:40 * e + 40], ht[320 + 40 * e:360 + 40 * e]], axis=0).astype(BF16)
    z_hid = swap(hs, hid_out)
    hid_out[z] = hs[z]

    arrived(b_up)
    i = at(0, 3)
    f_up = put(dbuf.at[i, c0], dbuf.at[i, c0], up_b)
    arrived(b_dn)
    i = at(0, 1)
    f_dn = put(dbuf.at[i, c1], dbuf.at[i, c1], down_b)
    sent[3] = spread(3)
    sent[1] = spread(1)
    fwd = {}

    def arrive(db):
        up, dn = sent[db]
        arrived(up)
        if db in (0, 2):
            i = at(3, db)
            fwd[db] = put(dbuf.at[i], dbuf.at[i], up_a)
        hand(3, db)
        arrived(dn)
        if db in (1, 3):
            i = at(1, db)
            fwd[db] = put(dbuf.at[i], dbuf.at[i], down_a)
        hand(1, db)

    def gradients(dd_of, first=False):
        def flip(r, carry):
            dd = dd_of(r)
            for j in range(7):
                v = dbuf[dd, 16 * j:16 * j + 16].astype(F32)
                dyr[pl.ds(pl.multiple_of(r * HALF + 16 * j, 16), 16)] = (
                    jnp.where(minus_at(dd, j), -v, v).astype(BF16))
            return carry

        lax.fori_loop(0, 4, flip, 0)
        dds = [dd_of(r) for r in range(4)]
        dy = jnp.concatenate([dbuf[dd] for dd in dds], axis=0)
        gmean = dot(jnp.concatenate([wm[dd] for dd in dds], axis=0), dy, TN)
        gpert = dot(jnp.concatenate([wd[dd] for dd in dds], axis=0), dyr[...], TN)
        if first:
            accm[...] = gmean
            accd[...] = gpert
        else:
            accm[...] += gmean
            accd[...] += gpert
        mx[:, 0:256] = dot(dy, ba[...])
        mx[:, 256:512] = dot(dyr[...], bb[...])

        def keep(r, carry):
            dd = dd_of(r)
            rows = pl.ds(pl.multiple_of(r * HALF, 16), HALF)
            for h in range(2):
                gt[2 * dd + h] = mx[rows, h * 128:(h + 1) * 128].astype(BF16)
                gdt[2 * dd + h] = mx[rows, 256 + h * 128:384 + h * 128]
            return carry

        lax.fori_loop(0, 4, keep, 0)

    def gradients_own(da, first=False):
        gradients(lambda r: at(da, r), first)

    def gradients_pair(db):
        for da in range(4):
            arrived(hands[db, da])
        gradients(lambda r: theirs(db, r))

    arrive(0)
    arrived(f_up)
    arrived(f_dn)
    sent[2] = spread(2)
    gradients_own(0, True)
    arrive(3)
    arrive(1)
    gradients_pair(0)
    arrive(2)
    gradients_own(3)
    arrived(fwd[0])
    hand(2, 0)
    gradients_own(1)
    arrived(fwd[3])
    hand(2, 3)
    arrived(fwd[1])
    hand(2, 1)
    gradients_pair(3)
    arrived(fwd[2])
    hand(2, 2)
    gradients_pair(1)
    gradients_own(2)
    gradients_pair(2)

    gp = accm[0:128, 0:320] + accm[128:256, 320:640]
    gn = accd[0:128, 0:320] + accd[128:256, 320:640]
    g = (gp + sgn_t[...] * gn).T
    for e in range(8):
        gs[e] = g[40 * e:40 * e + 40].astype(BF16)
    z_back = swap(gs, back_out)
    back_out[z] = gs[z]

    def store(i, ref, hbm, j):
        cols = pl.ds(pl.multiple_of(i * BLOCK, 128), BLOCK)
        return pltpu.make_async_copy(ref.at[:, cols], hbm.at[:, cols], local.at[2 * i + j])

    def turn(i, carry):
        cols = pl.ds(pl.multiple_of(i * BLOCK, 128), BLOCK)
        rows = pl.ds(8 * i, 8)
        gm[:, cols] = gt[rows].reshape(BLOCK, 128).T
        store(i, gm, gm_hbm, 0).start()
        gr[:, cols] = (gdt[rows].reshape(BLOCK, 128).T * noise[:, cols].astype(F32)
                       * jax.nn.sigmoid(rho[:, cols].astype(F32))).astype(BF16)
        store(i, gr, gr_hbm, 1).start()
        return carry

    lax.fori_loop(0, 8, turn, 0)
    for c in z_hid + z_back:
        arrived(c)

    def settle(i, carry):
        store(i, gm, gm_hbm, 0).wait()
        store(i, gr, gr_hbm, 1).wait()
        return carry

    lax.fori_loop(0, 8, settle, 0)
    for c in copies:
        if id(c) not in done:
            c.wait_recv()
    for c in copies:
        c.wait_send()
    assert len(copies) == COPIES


def layer(rows, words, cot, mean, rho, noise):
    v = pltpu.VMEM
    blk = lambda n: v((n, HALF, 640), BF16)
    one = v((HALF, 640), BF16)
    weight = v((128, UNITS), BF16)
    hbm = pl.BlockSpec(memory_space=pl.ANY)
    return pl.pallas_call(
        layer_kernel,
        in_specs=[VMEM] * 3 + [hbm] * 3,
        out_specs=[VMEM, VMEM, hbm, hbm],
        out_shape=[jax.ShapeDtypeStruct((8, 80, HALF), BF16), jax.ShapeDtypeStruct((8, 40, 128), BF16),
                   jax.ShapeDtypeStruct((128, UNITS), BF16), jax.ShapeDtypeStruct((128, UNITS), BF16)],
        scratch_shapes=[
            weight, weight, weight, v((32, HALF, 256), BF16), v((32, HALF, 256), BF16),
            v((8, 40, 128), BF16), v((8, 40, 128), I32), v((8, 40, 128), I32), v((8, 40, 224), BF16),
            v((2, 128, 640), I32), v((256, 640), BF16), v((256, 640), BF16),
            v((640, 256), BF16), v((640, 256), BF16), v((128, 320), F32), v((HALF, 640), F32),
            v((448, 640), F32), v((448, 640), F32),
            blk(32), blk(16), blk(16), blk(4), blk(4), blk(4), blk(3), one, one, one, blk(32),
            v((8, 80, HALF), BF16), v((448, 640), BF16), v((256, 640), F32), v((256, 640), F32),
            v((64, HALF, 128), BF16), v((64, HALF, 128), F32), v((8, 40, 128), BF16), weight, weight,
            pltpu.SemaphoreType.DMA((COPIES,)), pltpu.SemaphoreType.DMA((COPIES,)),
            pltpu.SemaphoreType.DMA((19,))],
        compiler_params=pltpu.CompilerParams(
            collective_id=1, has_side_effects=True, vmem_limit_bytes=62 * 1024 * 1024),
        name="layer",
    )(rows, words, cot, mean, rho, noise)


def bytes_of(words):
    parts = [(words >> (8 * j)) & 255 for j in range(4)]
    return jnp.concatenate(parts, axis=1).astype(F32).astype(BF16)


def words_of(parts):
    n = parts.shape[1] // 4
    ints = parts.astype(I32)
    return ints[:, :n] | (ints[:, n:2 * n] << 8) | (ints[:, 2 * n:3 * n] << 16) | (ints[:, 3 * n:] << 24)


def on_device(tokens, in_signs, out_signs, expert_ids, route_weight, cotangent,
              mean_weight, rho_weight, noise_weight):
    experts, capacity, slots, topk = 8, 40, 320, 2
    token_count = tokens.shape[0]
    core = lax.rem(lax.axis_index("dp"), 2)

    flat_ids = expert_ids.reshape(-1)
    pairs = token_count * topk
    onehot = (flat_ids[:, None] == jnp.arange(experts, dtype=I32)).astype(BF16)
    lower = (jnp.arange(pairs)[:, None] > jnp.arange(pairs)[None, :]).astype(BF16)
    before = dot(lower, onehot)
    ranks = jnp.sum(before * onehot.astype(F32), axis=1).astype(I32)
    slot_of = (flat_ids * capacity + ranks).reshape(token_count, topk)
    slot_ids = jnp.arange(slots, dtype=I32)
    picks = [slot_of[:, k][:, None] == slot_ids[None, :] for k in range(topk)]
    pick = [p.astype(BF16) for p in picks]
    gather = pick[0] + pick[1]
    slot_weight = sum(
        jnp.sum(jnp.where(p, route_weight[:, k][:, None], 0.0), axis=0) for k, p in enumerate(picks))

    half = lax.dynamic_slice_in_dim(out_signs, core * 112, 112, 1)
    half = jnp.concatenate([half, in_signs, jnp.zeros((token_count, 12), I32)], axis=1)
    send_rows = dot(gather, tokens, TN).astype(BF16)
    send_cot = (dot(gather, cotangent, TN) * slot_weight[:, None]).astype(BF16)
    send_words = words_of(dot(gather, bytes_of(half), TN))
    hid, back, grad_mean, grad_rho = layer(
        *(v.reshape(experts, capacity, -1) for v in (send_rows, send_words, send_cot)),
        mean_weight[0], rho_weight[0], noise_weight[0])
    w0, w1 = route_weight[:, 0:1], route_weight[:, 1:2]
    hidden_out = []
    for h in range(2):
        v = hid[:, 40 * h:40 * h + 40].reshape(slots, -1)
        hidden_out.append(dot(pick[0], v) * w0 + dot(pick[1], v) * w1)
    hidden_out = jnp.concatenate(hidden_out, axis=1).astype(BF16)
    grad_tokens = dot(gather, back.reshape(slots, -1)).astype(BF16)
    return hidden_out, grad_tokens, grad_mean[None], grad_rho[None]


def solution(mesh):
    row = P("expert", "dp")
    full = P("expert", None)
    weight = P("expert", "dp", None)
    return jax.shard_map(
        on_device, mesh=mesh,
        in_specs=(row, row, full, full, full, row, weight, weight, weight),
        out_specs=(row, row, weight, weight), check_vma=False)
```

```python
import jax
import jax.numpy as jnp
from jax import lax
from jax.experimental import pallas as pl
from jax.experimental.pallas import tpu as pltpu
from jax.sharding import PartitionSpec as P

F32 = jnp.float32
BF16 = jnp.bfloat16
I32 = jnp.int32
MESH = pl.DeviceIdType.MESH
NN = (((1,), (0,)), ((), ()))
TN = (((0,), (0,)), ((), ()))
VMEM = pl.BlockSpec(memory_space=pltpu.VMEM)

SIDE = 4
HALF = 112
OFFS = (2, 1, 3, 0)
CUT = ((0, 64), (64, 48))


NT = (((1,), (1,)), ((), ()))


def dot(a, b, dims=NN):
    return lax.dot_general(a, b, dims, preferred_element_type=F32)


VLIM = 50
ZORDER = (4, 3, 5, 2, 6, 1, 7)
UNITS = 7168
BLOCK = 896
COPIES = 35 + 1 + 16 + 12 + 6 + 2 + 2 + 8 + 4 + 16


def layer_kernel(tokens, in_signs, out_signs, ids, route, cotangent, mean_hbm, rho_hbm, noise_hbm,
                 hidden_out, grad_tokens, gm, gr,
                 picks, rows_in, words_in, cot_in, hid_out, back_out, mean, rho, noise, wm, wd, rows_r, words_r, words_p, cot_r, w2, bda, bdb, ba, bb, sgn_t,
                 up2, mx, dx, p, r0, q, t1, rp, rm, s, t2, rp2, rm2, dbuf, hs, dyr, accm, accd,
                 gt, gdt, gs, send, recv, local):
    me, z = lax.axis_index("dp"), lax.axis_index("expert")
    k = lax.rem(me, 2)
    x, y = me // 8, lax.rem(me // 2, SIDE)
    a, b = x * (1 - k) + y * k, y * (1 - k) + x * k
    sa, sb = 8 - 6 * k, 2 + 6 * k
    partner = me + 1 - 2 * k

    def at(da, db):
        return lax.rem(a + da, SIDE) * sa + lax.rem(b + db, SIDE) * sb + k

    def theirs(db, da):
        return lax.rem(b + db, SIDE) * sb + lax.rem(a + da, SIDE) * sa + (1 - k)

    up_a, down_a, up_b, down_b = at(1, 0), at(3, 0), at(0, 1), at(0, 3)

    loads = [pltpu.make_async_copy(src, dst, local.at[i]) for i, (src, dst) in enumerate(
        ((rho_hbm, rho), (noise_hbm, noise), (mean_hbm, mean)))]
    for c in loads:
        c.start()
    barrier = pltpu.get_barrier_semaphore()
    for o in ZORDER:
        pl.semaphore_signal(barrier, inc=1, device_id={"expert": lax.rem(z + o, 8)}, device_id_type=MESH)
    for peer in (up_a, down_a, up_b, down_b, partner):
        pl.semaphore_signal(barrier, inc=1, device_id={"dp": peer}, device_id_type=MESH)

    lane128 = lax.broadcasted_iota(I32, (128, 128), 1)
    row128 = lax.broadcasted_iota(I32, (128, 128), 0)
    names = [jnp.broadcast_to(ids[c:c + 1, :], (128, 128)) == row128 for c in range(2)]
    named = jnp.where(names[0] | names[1], 1.0, 0.0).astype(BF16)
    before = dot(named, jnp.where(row128 < lane128, 1.0, 0.0).astype(BF16))
    row320 = lax.broadcasted_iota(I32, (320, 128), 0)
    hit = []
    for c in range(2):
        rank = jnp.sum(jnp.where(names[c], before, 0.0), axis=0, keepdims=True).astype(I32)
        hit.append(jnp.broadcast_to(ids[c:c + 1, :] * 40 + rank, (320, 128)) == row320)
        picks[c] = jnp.where(hit[c], 1.0, 0.0).astype(BF16)
    gather_t = jnp.where(hit[0] | hit[1], 1.0, 0.0).astype(BF16)
    mine = jnp.where(k == 0, out_signs[0:112, :], out_signs[112:224, :])
    mine = jnp.concatenate([mine, in_signs[...], jnp.zeros((12, 128), I32)], axis=0)
    octets = jnp.concatenate(
        [((mine >> (8 * i)) & 255).astype(F32).astype(BF16) for i in range(4)], axis=0)
    octets = dot(gather_t, octets, NT).astype(I32)
    octets = (octets[:, 0:128] | (octets[:, 128:256] << 8)
              | (octets[:, 256:384] << 16) | (octets[:, 384:512] << 24))
    sent_rows = dot(gather_t, tokens[...])
    for e in range(8):
        words_in[e] = octets[40 * e:40 * e + 40]
        rows_in[e] = sent_rows[40 * e:40 * e + 40].astype(BF16)
    pl.semaphore_wait(barrier, 12)

    copies, done = [], set()

    def put(src, dst, to, axis="dp"):
        i = len(copies)
        c = pltpu.make_async_remote_copy(
            src, dst, send.at[i], recv.at[i], device_id={axis: to}, device_id_type=MESH)
        c.start()
        copies.append(c)
        return c

    def arrived(c):
        done.add(id(c))
        c.wait_recv()

    def swap(src, dst):
        out = []
        for o in ZORDER:
            to = lax.rem(z + o, 8)
            out.append(put(src.at[to], dst.at[z], to, "expert"))
        return out

    z_words = swap(words_in, words_r)
    z_rows = swap(rows_in, rows_r)
    weight_t = jnp.where(hit[0], route[0:1, :], 0.0) + jnp.where(hit[1], route[1:2, :], 0.0)
    sent_cot = dot(gather_t, cotangent[...], NT) * jnp.sum(weight_t, axis=1, keepdims=True)
    for e in range(8):
        cot_in[e] = sent_cot[40 * e:40 * e + 40].astype(BF16)
    z_cot = swap(cot_in, cot_r)
    words_r[z] = words_in[z]
    rows_r[z] = rows_in[z]
    cot_r[z] = cot_in[z]

    for c in loads:
        c.wait()

    def fold(i, carry):
        cols = pl.ds(pl.multiple_of(i * BLOCK, 128), BLOCK)
        delta = (jax.nn.softplus(rho[:, cols].astype(F32)) * noise[:, cols].astype(F32)).astype(BF16)
        for v, wt in ((mean[:, cols], wm), (delta, wd)):
            t = v.T
            for d in range(4):
                for h in range(2):
                    o = (2 * d + h) * HALF
                    wt[4 * i + d, :, h * 128:(h + 1) * 128] = t[o:o + HALF]
        return carry

    lax.fori_loop(0, 8, fold, 0)

    def slots_of(ref):
        return jnp.concatenate([ref[e].astype(F32) for e in range(8)], axis=0)

    for c in z_words:
        arrived(c)
    pair_words = put(words_r, words_p, partner)
    words = jnp.concatenate([words_r[e] for e in range(8)], axis=0)
    wt = words.T
    w2[k] = jnp.concatenate([wt, wt], axis=1)
    lane = lax.broadcasted_iota(I32, (320, 128), 1)
    word = jnp.broadcast_to(words[:, 115:116], (320, 128))
    for w in range(3):
        word = jnp.where(lane // 32 == w, jnp.broadcast_to(words[:, 112 + w:113 + w], (320, 128)), word)
    sgn = (1 - 2 * ((word >> (lane & 31)) & 1)).astype(F32)
    for c in z_rows:
        arrived(c)
    plain = slots_of(rows_r)
    signed = plain * sgn
    sgn_t[...] = sgn.T
    none_w, none_t = jnp.zeros((128, 320), F32), jnp.zeros((320, 128), F32)
    for v, wide, tall in ((plain, bda, ba), (signed, bdb, bb)):
        t = v.T
        wide[0:128] = jnp.concatenate([t, none_w], axis=1).astype(BF16)
        wide[128:256] = jnp.concatenate([none_w, t], axis=1).astype(BF16)
        tall[0:320] = jnp.concatenate([v, none_t], axis=1).astype(BF16)
        tall[320:640] = jnp.concatenate([none_t, v], axis=1).astype(BF16)
    arrived(pair_words)
    wt = jnp.concatenate([words_p[e] for e in range(8)], axis=0).T
    w2[1 - k] = jnp.concatenate([wt, wt], axis=1)

    left = lax.broadcasted_iota(I32, (1, 640), 1) < 320
    down16 = lax.broadcasted_iota(I32, (16, 640), 0)

    def minus_at(dd, j):
        half, base = dd // 16, lax.rem(dd, 16) * 7
        one = w2[half, pl.ds(base + j // 2, 1), :] >> (16 * (j % 2))
        two = w2[half, pl.ds(base + 3 + (j + 1) // 2, 1), :] >> (16 * ((j + 1) % 2))
        return ((jnp.broadcast_to(jnp.where(left, one, two), (16, 640)) >> down16) & 1) != 0

    def products(dd_of):
        mx[...] = dot(jnp.concatenate([wm[dd_of(r)] for r in range(4)], axis=0), bda[...])
        dx[...] = dot(jnp.concatenate([wd[dd_of(r)] for r in range(4)], axis=0), bdb[...])

        for r in range(4):
            dd = dd_of(r)
            for j in range(7):
                o = r * HALF + 16 * j
                pert = dx[o:o + 16]
                p[dd, 16 * j:16 * j + 16] = (
                    mx[o:o + 16] + jnp.where(minus_at(dd, j), -pert, pert)).astype(BF16)

    pair = {}

    def products_pair(g):
        products(lambda r: theirs(OFFS[g], r))
        for r in range(4):
            pair[g, r] = put(p.at[theirs(OFFS[g], OFFS[r])], r0.at[4 * g + r], partner)

    def products_own(g):
        products(lambda r: at(OFFS[g], r))

    def merge(g, r):
        arrived(pair[g, r])
        q[4 * g + r] = p[at(OFFS[g], OFFS[r])] + r0[4 * g + r]

    def qq(g, r):
        return q.at[4 * g + r]

    far, plus, minus = {}, {}, {}
    products_pair(0)
    products_own(0)
    products_pair(1)
    for r in range(4):
        merge(0, r)
        far[r] = put(qq(0, r), t1.at[r], up_a if r in (0, 3) else down_a)
    products_pair(2)
    products_own(1)
    products_own(2)

    def relay(r):
        arrived(far[r])
        g = 1 if r in (0, 3) else 2
        q[4 * g + r] = q[4 * g + r] + t1[r]
        if g == 1:
            plus[r] = put(qq(1, r), rp.at[r], up_a)
        else:
            minus[r] = put(qq(2, r), rm.at[r], down_a)

    merge(2, 0)
    minus[0] = put(qq(2, 0), rm.at[0], down_a)
    merge(1, 0)
    relay(0)
    merge(1, 1)
    plus[1] = put(qq(1, 1), rp.at[1], up_a)
    merge(2, 1)
    relay(1)
    merge(1, 2)
    plus[2] = put(qq(1, 2), rp.at[2], up_a)
    merge(2, 2)
    relay(2)
    merge(2, 3)
    minus[3] = put(qq(2, 3), rm.at[3], down_a)
    merge(1, 3)
    relay(3)
    products_pair(3)
    products_own(3)
    for c in z_cot:
        arrived(c)
    ut = slots_of(cot_r).T
    up2[...] = jnp.concatenate([ut[:HALF], ut[HALF:]], axis=1)
    for r in range(4):
        merge(3, r)

    def total(r):
        arrived(plus[r])
        arrived(minus[r])
        return q[12 + r].astype(F32) + rp[r].astype(F32) + rm[r].astype(F32)

    (o0, n0), (o1, n1) = CUT
    c0, c1 = pl.ds(o0, n0), pl.ds(o1, n1)
    s[0] = total(0).astype(BF16)
    far_up = put(s.at[0, c0], t2.at[c0], up_b)
    far_dn = put(s.at[0, c1], t2.at[c1], down_b)
    s[1] = total(1).astype(BF16)
    p1 = put(s.at[1, c1], rp2.at[c1], up_b)
    s[2] = total(2).astype(BF16)
    m1 = put(s.at[2, c0], rm2.at[c0], down_b)
    arrived(far_up)
    s[1, c0] = s[1, c0] + t2[c0]
    p2 = put(s.at[1, c0], rp2.at[c0], up_b)
    arrived(far_dn)
    s[2, c1] = s[2, c1] + t2[c1]
    m2 = put(s.at[2, c1], rm2.at[c1], down_b)
    own = total(3)
    for c in (p1, m1, p2, m2):
        arrived(c)

    pre = own + rp2[...].astype(F32) + rm2[...].astype(F32)
    gate = jax.nn.sigmoid(pre)
    slope = gate * (1.0 + pre * (1.0 - gate))
    dbuf[me] = (up2[...] * slope).astype(BF16)

    def hand(da, db):
        i = at(da, db)
        hands[da, db] = put(dbuf.at[i], dbuf.at[i], partner)

    def spread(db):
        i = at(0, db)
        up = put(dbuf.at[i], dbuf.at[i], up_a)
        dn = put(dbuf.at[i], dbuf.at[i], down_a)
        hand(0, db)
        return up, dn

    hands = {}
    b_up = put(dbuf.at[me], dbuf.at[me], up_b)
    b_dn = put(dbuf.at[me], dbuf.at[me], down_b)
    sent = {0: spread(0)}

    ht = (pre * gate).T
    for e in range(8):
        hs[e] = jnp.concatenate(
            [ht[40 * e:40 * e + 40], ht[320 + 40 * e:360 + 40 * e]], axis=0).astype(BF16)
    z_hid = swap(hs, hid_out)
    hid_out[z] = hs[z]

    arrived(b_up)
    i = at(0, 3)
    f_up = put(dbuf.at[i, c0], dbuf.at[i, c0], up_b)
    arrived(b_dn)
    i = at(0, 1)
    f_dn = put(dbuf.at[i, c1], dbuf.at[i, c1], down_b)
    sent[3] = spread(3)
    sent[1] = spread(1)
    fwd = {}

    def arrive(db):
        up, dn = sent[db]
        arrived(up)
        if db in (0, 2):
            i = at(3, db)
            fwd[db] = put(dbuf.at[i], dbuf.at[i], up_a)
        hand(3, db)
        arrived(dn)
        if db in (1, 3):
            i = at(1, db)
            fwd[db] = put(dbuf.at[i], dbuf.at[i], down_a)
        hand(1, db)

    def gradients(dd_of, first=False):
        for r in range(4):
            dd = dd_of(r)
            for j in range(7):
                o = r * HALF + 16 * j
                v = dbuf[dd, 16 * j:16 * j + 16].astype(F32)
                dyr[o:o + 16] = jnp.where(minus_at(dd, j), -v, v).astype(BF16)
        dds = [dd_of(r) for r in range(4)]
        dy = jnp.concatenate([dbuf[dd] for dd in dds], axis=0)
        gmean = dot(jnp.concatenate([wm[dd] for dd in dds], axis=0), dy, TN)
        gpert = dot(jnp.concatenate([wd[dd] for dd in dds], axis=0), dyr[...], TN)
        if first:
            accm[...] = gmean
            accd[...] = gpert
        else:
            accm[...] += gmean
            accd[...] += gpert
        mx[:, 0:256] = dot(dy, ba[...])
        mx[:, 256:512] = dot(dyr[...], bb[...])

        def keep(r, carry):
            dd = dd_of(r)
            rows = pl.ds(pl.multiple_of(r * HALF, 16), HALF)
            for h in range(2):
                gt[2 * dd + h] = mx[rows, h * 128:(h + 1) * 128].astype(BF16)
                gdt[2 * dd + h] = mx[rows, 256 + h * 128:384 + h * 128]
            return carry

        lax.fori_loop(0, 4, keep, 0)

    def gradients_own(da, first=False):
        gradients(lambda r: at(da, r), first)

    def gradients_pair(db):
        for da in range(4):
            arrived(hands[db, da])
        gradients(lambda r: theirs(db, r))

    arrived(f_up)
    arrived(f_dn)
    sent[2] = spread(2)
    arrive(0)
    gradients_own(0, True)
    arrive(3)
    arrive(1)
    gradients_pair(0)
    arrive(2)
    gradients_own(3)
    arrived(fwd[0])
    hand(2, 0)
    gradients_own(1)
    arrived(fwd[3])
    hand(2, 3)
    arrived(fwd[1])
    hand(2, 1)
    gradients_pair(3)
    arrived(fwd[2])
    hand(2, 2)
    gradients_pair(1)
    gradients_own(2)
    gradients_pair(2)

    gp = accm[0:128, 0:320] + accm[128:256, 320:640]
    gn = accd[0:128, 0:320] + accd[128:256, 320:640]
    g = (gp + sgn_t[...] * gn).T
    for e in range(8):
        gs[e] = g[40 * e:40 * e + 40].astype(BF16)
    z_back = swap(gs, back_out)
    back_out[z] = gs[z]

    def turn(i, carry):
        cols = pl.ds(pl.multiple_of(i * BLOCK, 128), BLOCK)
        rows = pl.ds(8 * i, 8)
        gm[:, cols] = gt[rows].reshape(BLOCK, 128).T
        gr[:, cols] = (gdt[rows].reshape(BLOCK, 128).T * noise[:, cols].astype(F32)
                       * jax.nn.sigmoid(rho[:, cols].astype(F32))).astype(BF16)
        return carry

    lax.fori_loop(0, 8, turn, 0)
    for c in z_hid:
        arrived(c)
    for h in range(2):
        v = jnp.concatenate(
            [hid_out[e].astype(F32)[40 * h:40 * h + 40] for e in range(8)], axis=0).astype(BF16)
        hidden_out[HALF * h:HALF * h + HALF] = (
            dot(v, picks[0], TN) * route[0:1, :] + dot(v, picks[1], TN) * route[1:2, :]).astype(BF16)
    for c in z_back:
        arrived(c)
    grad_tokens[...] = dot(picks[0] + picks[1], slots_of(back_out).astype(BF16), TN).astype(BF16)

    for c in copies:
        if id(c) not in done:
            c.wait_recv()
    for c in copies:
        c.wait_send()
    assert len(copies) == COPIES


def layer(*args):
    v = pltpu.VMEM
    blk = lambda n: v((n, HALF, 640), BF16)
    one = v((HALF, 640), BF16)
    weight = v((128, UNITS), BF16)
    hbm = pl.BlockSpec(memory_space=pltpu.HBM)
    return pl.pallas_call(
        layer_kernel,
        in_specs=[VMEM] * 6 + [hbm] * 3,
        out_specs=[VMEM] * 4,
        out_shape=[jax.ShapeDtypeStruct((224, 128), BF16), jax.ShapeDtypeStruct((128, 128), BF16),
                   jax.ShapeDtypeStruct((128, UNITS), BF16), jax.ShapeDtypeStruct((128, UNITS), BF16)],
        scratch_shapes=[
            v((2, 320, 128), BF16), v((8, 40, 128), BF16), v((8, 40, 128), I32), v((8, 40, 224), BF16),
            v((8, 80, HALF), BF16), v((8, 40, 128), BF16),
            weight, weight, weight, v((32, HALF, 256), BF16), v((32, HALF, 256), BF16),
            v((8, 40, 128), BF16), v((8, 40, 128), I32), v((8, 40, 128), I32), v((8, 40, 224), BF16),
            v((2, 128, 640), I32), v((256, 640), BF16), v((256, 640), BF16),
            v((640, 256), BF16), v((640, 256), BF16), v((128, 320), F32), v((HALF, 640), F32),
            v((448, 640), F32), v((448, 640), F32),
            blk(32), blk(16), blk(16), blk(4), blk(4), blk(4), blk(3), one, one, one, blk(32),
            v((8, 80, HALF), BF16), v((448, 640), BF16), v((256, 640), F32), v((256, 640), F32),
            v((64, HALF, 128), BF16), v((64, HALF, 128), F32), v((8, 40, 128), BF16),
            pltpu.SemaphoreType.DMA((COPIES,)), pltpu.SemaphoreType.DMA((COPIES,)),
            pltpu.SemaphoreType.DMA((3,))],
        compiler_params=pltpu.CompilerParams(
            collective_id=1, has_side_effects=True, vmem_limit_bytes=VLIM * 1024 * 1024),
        name="layer",
    )(*args)


def on_device(tokens, in_signs, out_signs, expert_ids, route_weight, cotangent,
              mean_weight, rho_weight, noise_weight):
    hidden_out, grad_tokens, grad_mean, grad_rho = layer(
        tokens, in_signs.T, out_signs.T, expert_ids.T, route_weight.T, cotangent.T,
        mean_weight[0], rho_weight[0], noise_weight[0])
    return hidden_out.T, grad_tokens, grad_mean[None], grad_rho[None]


def solution(mesh):
    row = P("expert", "dp")
    full = P("expert", None)
    weight = P("expert", "dp", None)
    return jax.shard_map(
        on_device, mesh=mesh,
        in_specs=(row, row, full, full, full, row, weight, weight, weight),
        out_specs=(row, row, weight, weight), check_vma=False)
```

```python
import jax
import jax.numpy as jnp
from jax import lax
from jax.experimental import pallas as pl
from jax.experimental.pallas import tpu as pltpu
from jax.sharding import PartitionSpec as P

F32 = jnp.float32
BF16 = jnp.bfloat16
I32 = jnp.int32
MESH = pl.DeviceIdType.MESH
NN = (((1,), (0,)), ((), ()))
TN = (((0,), (0,)), ((), ()))
VMEM = pl.BlockSpec(memory_space=pltpu.VMEM)

SIDE = 4
HALF = 112
OFFS = (2, 1, 3, 0)
CUT = ((0, 64), (64, 48))


NT = (((1,), (1,)), ((), ()))


def dot(a, b, dims=NN):
    return lax.dot_general(a, b, dims, preferred_element_type=F32)


VLIM = 50
ZORDER = (4, 3, 5, 2, 6, 1, 7)
UNITS = 7168
BLOCK = 896
COPIES = 35 + 1 + 16 + 24 + 6 + 2 + 2 + 8 + 8 + 16


def layer_kernel(tokens_hbm, ins_hbm, outs_hbm, ids_hbm, route_hbm, cot_hbm, mean_hbm, rho_hbm, noise_hbm,
                 hidden_out, grad_tokens, gm, gr,
                 tokens, in_signs, out_signs, ids, route, cotangent, picks, rows_in, words_in, cot_in, hid_out, back_out, mean, rho, noise, wm, wd, rows_r, words_r, words_p, cot_r, w2, bda, bdb, ba, bb, sgn_t,
                 up2, mx, dx, p, r0, q, t1, rp, rm, s, t2, rp2, rm2, dbuf, hs, dyr, accm, accd,
                 gt, gdt, gs, send, recv, local):
    me, z = lax.axis_index("dp"), lax.axis_index("expert")
    k = lax.rem(me, 2)
    x, y = me // 8, lax.rem(me // 2, SIDE)
    a, b = x * (1 - k) + y * k, y * (1 - k) + x * k
    sa, sb = 8 - 6 * k, 2 + 6 * k
    partner = me + 1 - 2 * k

    def at(da, db):
        return lax.rem(a + da, SIDE) * sa + lax.rem(b + db, SIDE) * sb + k

    def theirs(db, da):
        return lax.rem(b + db, SIDE) * sb + lax.rem(a + da, SIDE) * sa + (1 - k)

    up_a, down_a, up_b, down_b = at(1, 0), at(3, 0), at(0, 1), at(0, 3)

    loads = [pltpu.make_async_copy(src, dst, local.at[i]) for i, (src, dst) in enumerate(
        ((rho_hbm, rho), (noise_hbm, noise), (mean_hbm, mean), (ids_hbm, ids), (outs_hbm, out_signs),
         (ins_hbm, in_signs), (tokens_hbm, tokens), (route_hbm, route), (cot_hbm, cotangent)))]
    for c in loads[3:] + loads[:3]:
        c.start()
    barrier = pltpu.get_barrier_semaphore()
    for o in ZORDER:
        pl.semaphore_signal(barrier, inc=1, device_id={"expert": lax.rem(z + o, 8)}, device_id_type=MESH)
    for peer in (up_a, down_a, up_b, down_b, partner):
        pl.semaphore_signal(barrier, inc=1, device_id={"dp": peer}, device_id_type=MESH)

    for c in loads[3:]:
        c.wait()
    lane128 = lax.broadcasted_iota(I32, (128, 128), 1)
    row128 = lax.broadcasted_iota(I32, (128, 128), 0)
    names = [jnp.broadcast_to(ids[c:c + 1, :], (128, 128)) == row128 for c in range(2)]
    named = jnp.where(names[0] | names[1], 1.0, 0.0).astype(BF16)
    before = dot(named, jnp.where(row128 < lane128, 1.0, 0.0).astype(BF16))
    row320 = lax.broadcasted_iota(I32, (320, 128), 0)
    hit = []
    for c in range(2):
        rank = jnp.sum(jnp.where(names[c], before, 0.0), axis=0, keepdims=True).astype(I32)
        hit.append(jnp.broadcast_to(ids[c:c + 1, :] * 40 + rank, (320, 128)) == row320)
        picks[c] = jnp.where(hit[c], 1.0, 0.0).astype(BF16)
    gather_t = jnp.where(hit[0] | hit[1], 1.0, 0.0).astype(BF16)
    mine = jnp.where(k == 0, out_signs[0:112, :], out_signs[112:224, :])
    mine = jnp.concatenate([mine, in_signs[...], jnp.zeros((12, 128), I32)], axis=0)
    octets = jnp.concatenate(
        [((mine >> (8 * i)) & 255).astype(F32).astype(BF16) for i in range(4)], axis=0)
    octets = dot(gather_t, octets, NT).astype(I32)
    octets = (octets[:, 0:128] | (octets[:, 128:256] << 8)
              | (octets[:, 256:384] << 16) | (octets[:, 384:512] << 24))
    sent_rows = dot(gather_t, tokens[...])
    for e in range(8):
        words_in[e] = octets[40 * e:40 * e + 40]
        rows_in[e] = sent_rows[40 * e:40 * e + 40].astype(BF16)
    pl.semaphore_wait(barrier, 12)

    copies, done = [], set()

    def put(src, dst, to, axis="dp"):
        i = len(copies)
        c = pltpu.make_async_remote_copy(
            src, dst, send.at[i], recv.at[i], device_id={axis: to}, device_id_type=MESH)
        c.start()
        copies.append(c)
        return c

    def arrived(c):
        done.add(id(c))
        c.wait_recv()

    def swap(src, dst):
        out = []
        for o in ZORDER:
            to = lax.rem(z + o, 8)
            out.append(put(src.at[to], dst.at[z], to, "expert"))
        return out

    z_words = swap(words_in, words_r)
    z_rows = swap(rows_in, rows_r)
    weight_t = jnp.where(hit[0], route[0:1, :], 0.0) + jnp.where(hit[1], route[1:2, :], 0.0)
    sent_cot = dot(gather_t, cotangent[...], NT) * jnp.sum(weight_t, axis=1, keepdims=True)
    for e in range(8):
        cot_in[e] = sent_cot[40 * e:40 * e + 40].astype(BF16)
    z_cot = swap(cot_in, cot_r)
    words_r[z] = words_in[z]
    rows_r[z] = rows_in[z]
    cot_r[z] = cot_in[z]

    for c in loads[:3]:
        c.wait()

    def fold(i, carry):
        cols = pl.ds(pl.multiple_of(i * BLOCK, 128), BLOCK)
        delta = (jax.nn.softplus(rho[:, cols].astype(F32)) * noise[:, cols].astype(F32)).astype(BF16)
        for v, wt in ((mean[:, cols], wm), (delta, wd)):
            t = v.T
            for d in range(4):
                for h in range(2):
                    o = (2 * d + h) * HALF
                    wt[4 * i + d, :, h * 128:(h + 1) * 128] = t[o:o + HALF]
        return carry

    lax.fori_loop(0, 8, fold, 0)

    def slots_of(ref):
        return jnp.concatenate([ref[e].astype(F32) for e in range(8)], axis=0)

    for c in z_words:
        arrived(c)
    pair_words = put(words_r, words_p, partner)
    words = jnp.concatenate([words_r[e] for e in range(8)], axis=0)
    wt = words.T
    w2[k] = jnp.concatenate([wt, wt], axis=1)
    lane = lax.broadcasted_iota(I32, (320, 128), 1)
    word = jnp.broadcast_to(words[:, 115:116], (320, 128))
    for w in range(3):
        word = jnp.where(lane // 32 == w, jnp.broadcast_to(words[:, 112 + w:113 + w], (320, 128)), word)
    sgn = (1 - 2 * ((word >> (lane & 31)) & 1)).astype(F32)
    for c in z_rows:
        arrived(c)
    plain = slots_of(rows_r)
    signed = plain * sgn
    sgn_t[...] = sgn.T
    none_w, none_t = jnp.zeros((128, 320), F32), jnp.zeros((320, 128), F32)
    for v, wide, tall in ((plain, bda, ba), (signed, bdb, bb)):
        t = v.T
        wide[0:128] = jnp.concatenate([t, none_w], axis=1).astype(BF16)
        wide[128:256] = jnp.concatenate([none_w, t], axis=1).astype(BF16)
        tall[0:320] = jnp.concatenate([v, none_t], axis=1).astype(BF16)
        tall[320:640] = jnp.concatenate([none_t, v], axis=1).astype(BF16)
    arrived(pair_words)
    wt = jnp.concatenate([words_p[e] for e in range(8)], axis=0).T
    w2[1 - k] = jnp.concatenate([wt, wt], axis=1)

    left = lax.broadcasted_iota(I32, (1, 640), 1) < 320
    down16 = lax.broadcasted_iota(I32, (16, 640), 0)

    def minus_at(dd, j):
        half, base = dd // 16, lax.rem(dd, 16) * 7
        one = w2[half, pl.ds(base + j // 2, 1), :] >> (16 * (j % 2))
        two = w2[half, pl.ds(base + 3 + (j + 1) // 2, 1), :] >> (16 * ((j + 1) % 2))
        return ((jnp.broadcast_to(jnp.where(left, one, two), (16, 640)) >> down16) & 1) != 0

    def products(dd_of):
        mx[...] = dot(jnp.concatenate([wm[dd_of(r)] for r in range(4)], axis=0), bda[...])
        dx[...] = dot(jnp.concatenate([wd[dd_of(r)] for r in range(4)], axis=0), bdb[...])

        for r in range(4):
            dd = dd_of(r)
            for j in range(7):
                o = r * HALF + 16 * j
                pert = dx[o:o + 16]
                p[dd, 16 * j:16 * j + 16] = (
                    mx[o:o + 16] + jnp.where(minus_at(dd, j), -pert, pert)).astype(BF16)

    pair = {}

    def products_pair(g):
        products(lambda r: theirs(OFFS[g], r))
        for r in range(4):
            pair[g, r] = put(p.at[theirs(OFFS[g], OFFS[r])], r0.at[4 * g + r], partner)

    def products_own(g):
        products(lambda r: at(OFFS[g], r))

    def merge(g, r):
        arrived(pair[g, r])
        q[4 * g + r] = p[at(OFFS[g], OFFS[r])] + r0[4 * g + r]

    far, plus, minus = {}, {}, {}
    (o0, n0), (o1, n1) = CUT
    c0, c1 = pl.ds(o0, n0), pl.ds(o1, n1)
    products_pair(0)
    products_own(0)
    products_pair(1)
    for r in range(4):
        merge(0, r)
        far[r] = (put(q.at[r, c0], t1.at[r, c0], up_a), put(q.at[r, c1], t1.at[r, c1], down_a))
    products_pair(2)
    products_own(1)
    products_own(2)
    products_pair(3)
    products_own(3)

    def relay(r):
        merge(1, r)
        plus[r] = [put(q.at[4 + r, c1], rp.at[r, c1], up_a)]
        merge(2, r)
        minus[r] = [put(q.at[8 + r, c0], rm.at[r, c0], down_a)]
        up, dn = far[r]
        arrived(up)
        q[4 + r, c0] = q[4 + r, c0] + t1[r, c0]
        plus[r].append(put(q.at[4 + r, c0], rp.at[r, c0], up_a))
        arrived(dn)
        q[8 + r, c1] = q[8 + r, c1] + t1[r, c1]
        minus[r].append(put(q.at[8 + r, c1], rm.at[r, c1], down_a))

    for r in range(4):
        relay(r)
    for c in z_cot:
        arrived(c)
    ut = slots_of(cot_r).T
    up2[...] = jnp.concatenate([ut[:HALF], ut[HALF:]], axis=1)
    for r in range(4):
        merge(3, r)

    def total(r):
        for c in plus[r] + minus[r]:
            arrived(c)
        return q[12 + r].astype(F32) + rp[r].astype(F32) + rm[r].astype(F32)

    s[0] = total(0).astype(BF16)
    far_up = put(s.at[0, c0], t2.at[c0], up_b)
    far_dn = put(s.at[0, c1], t2.at[c1], down_b)
    s[1] = total(1).astype(BF16)
    p1 = put(s.at[1, c1], rp2.at[c1], up_b)
    s[2] = total(2).astype(BF16)
    m1 = put(s.at[2, c0], rm2.at[c0], down_b)
    arrived(far_up)
    s[1, c0] = s[1, c0] + t2[c0]
    p2 = put(s.at[1, c0], rp2.at[c0], up_b)
    arrived(far_dn)
    s[2, c1] = s[2, c1] + t2[c1]
    m2 = put(s.at[2, c1], rm2.at[c1], down_b)
    own = total(3)
    for c in (p1, m1, p2, m2):
        arrived(c)

    pre = own + rp2[...].astype(F32) + rm2[...].astype(F32)
    gate = jax.nn.sigmoid(pre)
    slope = gate * (1.0 + pre * (1.0 - gate))
    dbuf[me] = (up2[...] * slope).astype(BF16)

    def hand(da, db):
        i = at(da, db)
        hands[da, db] = put(dbuf.at[i], dbuf.at[i], partner)

    def spread(db):
        i = at(0, db)
        up = put(dbuf.at[i], dbuf.at[i], up_a)
        dn = put(dbuf.at[i], dbuf.at[i], down_a)
        hand(0, db)
        return up, dn

    hands = {}
    b_up = put(dbuf.at[me], dbuf.at[me], up_b)
    b_dn = put(dbuf.at[me], dbuf.at[me], down_b)
    sent = {0: spread(0)}

    ht = (pre * gate).T
    for e in range(8):
        hs[e] = jnp.concatenate(
            [ht[40 * e:40 * e + 40], ht[320 + 40 * e:360 + 40 * e]], axis=0).astype(BF16)
    z_hid = swap(hs, hid_out)
    hid_out[z] = hs[z]

    arrived(b_up)
    i = at(0, 3)
    f_up = put(dbuf.at[i, c0], dbuf.at[i, c0], up_b)
    arrived(b_dn)
    i = at(0, 1)
    f_dn = put(dbuf.at[i, c1], dbuf.at[i, c1], down_b)
    sent[3] = spread(3)
    sent[1] = spread(1)
    fwd = {}

    def arrive(db):
        up, dn = sent[db]
        arrived(up)
        i = at(3, db)
        fwd[db] = [put(dbuf.at[i, c0], dbuf.at[i, c0], up_a)]
        hand(3, db)
        arrived(dn)
        i = at(1, db)
        fwd[db].append(put(dbuf.at[i, c1], dbuf.at[i, c1], down_a))
        hand(1, db)

    def last(db):
        for c in fwd[db]:
            arrived(c)
        hand(2, db)

    def gradients(dd_of, first=False):
        for r in range(4):
            dd = dd_of(r)
            for j in range(7):
                o = r * HALF + 16 * j
                v = dbuf[dd, 16 * j:16 * j + 16].astype(F32)
                dyr[o:o + 16] = jnp.where(minus_at(dd, j), -v, v).astype(BF16)
        dds = [dd_of(r) for r in range(4)]
        dy = jnp.concatenate([dbuf[dd] for dd in dds], axis=0)
        gmean = dot(jnp.concatenate([wm[dd] for dd in dds], axis=0), dy, TN)
        gpert = dot(jnp.concatenate([wd[dd] for dd in dds], axis=0), dyr[...], TN)
        if first:
            accm[...] = gmean
            accd[...] = gpert
        else:
            accm[...] += gmean
            accd[...] += gpert
        mx[:, 0:256] = dot(dy, ba[...])
        mx[:, 256:512] = dot(dyr[...], bb[...])

        def keep(r, carry):
            dd = dd_of(r)
            rows = pl.ds(pl.multiple_of(r * HALF, 16), HALF)
            for h in range(2):
                gt[2 * dd + h] = mx[rows, h * 128:(h + 1) * 128].astype(BF16)
                gdt[2 * dd + h] = mx[rows, 256 + h * 128:384 + h * 128]
            return carry

        lax.fori_loop(0, 4, keep, 0)

    def gradients_own(da, first=False):
        gradients(lambda r: at(da, r), first)

    def gradients_pair(db):
        for da in range(4):
            arrived(hands[db, da])
        gradients(lambda r: theirs(db, r))

    arrived(f_up)
    arrived(f_dn)
    sent[2] = spread(2)
    arrive(0)
    gradients_own(0, True)
    arrive(3)
    arrive(1)
    gradients_pair(0)
    arrive(2)
    gradients_own(3)
    last(0)
    gradients_own(1)
    last(3)
    last(1)
    gradients_pair(3)
    last(2)
    gradients_pair(1)
    gradients_own(2)
    gradients_pair(2)

    gp = accm[0:128, 0:320] + accm[128:256, 320:640]
    gn = accd[0:128, 0:320] + accd[128:256, 320:640]
    g = (gp + sgn_t[...] * gn).T
    for e in range(8):
        gs[e] = g[40 * e:40 * e + 40].astype(BF16)
    z_back = swap(gs, back_out)
    back_out[z] = gs[z]

    def turn(i, carry):
        cols = pl.ds(pl.multiple_of(i * BLOCK, 128), BLOCK)
        rows = pl.ds(8 * i, 8)
        gm[:, cols] = gt[rows].reshape(BLOCK, 128).T
        gr[:, cols] = (gdt[rows].reshape(BLOCK, 128).T * noise[:, cols].astype(F32)
                       * jax.nn.sigmoid(rho[:, cols].astype(F32))).astype(BF16)
        return carry

    lax.fori_loop(0, 8, turn, 0)
    for c in z_hid:
        arrived(c)
    for h in range(2):
        v = jnp.concatenate(
            [hid_out[e].astype(F32)[40 * h:40 * h + 40] for e in range(8)], axis=0).astype(BF16)
        hidden_out[HALF * h:HALF * h + HALF] = (
            dot(v, picks[0], TN) * route[0:1, :] + dot(v, picks[1], TN) * route[1:2, :]).astype(BF16)
    for c in z_back:
        arrived(c)
    grad_tokens[...] = dot(picks[0] + picks[1], slots_of(back_out).astype(BF16), TN).astype(BF16)

    for c in copies:
        if id(c) not in done:
            c.wait_recv()
    for c in copies:
        c.wait_send()
    assert len(copies) == COPIES


def layer(*args):
    v = pltpu.VMEM
    blk = lambda n: v((n, HALF, 640), BF16)
    one = v((HALF, 640), BF16)
    weight = v((128, UNITS), BF16)
    hbm = pl.BlockSpec(memory_space=pltpu.HBM)
    return pl.pallas_call(
        layer_kernel,
        in_specs=[hbm] * 9,
        out_specs=[VMEM] * 4,
        out_shape=[jax.ShapeDtypeStruct((224, 128), BF16), jax.ShapeDtypeStruct((128, 128), BF16),
                   jax.ShapeDtypeStruct((128, UNITS), BF16), jax.ShapeDtypeStruct((128, UNITS), BF16)],
        scratch_shapes=[
            v((128, 128), BF16), v((4, 128), I32), v((224, 128), I32), v((2, 128), I32), v((2, 128), F32),
            v((224, 128), BF16), v((2, 320, 128), BF16), v((8, 40, 128), BF16), v((8, 40, 128), I32), v((8, 40, 224), BF16),
            v((8, 80, HALF), BF16), v((8, 40, 128), BF16),
            weight, weight, weight, v((32, HALF, 256), BF16), v((32, HALF, 256), BF16),
            v((8, 40, 128), BF16), v((8, 40, 128), I32), v((8, 40, 128), I32), v((8, 40, 224), BF16),
            v((2, 128, 640), I32), v((256, 640), BF16), v((256, 640), BF16),
            v((640, 256), BF16), v((640, 256), BF16), v((128, 320), F32), v((HALF, 640), F32),
            v((448, 640), F32), v((448, 640), F32),
            blk(32), blk(16), blk(16), blk(4), blk(4), blk(4), blk(3), one, one, one, blk(32),
            v((8, 80, HALF), BF16), v((448, 640), BF16), v((256, 640), F32), v((256, 640), F32),
            v((64, HALF, 128), BF16), v((64, HALF, 128), F32), v((8, 40, 128), BF16),
            pltpu.SemaphoreType.DMA((COPIES,)), pltpu.SemaphoreType.DMA((COPIES,)),
            pltpu.SemaphoreType.DMA((9,))],
        compiler_params=pltpu.CompilerParams(
            collective_id=1, has_side_effects=True, vmem_limit_bytes=VLIM * 1024 * 1024),
        name="layer",
    )(*args)


def on_device(tokens, in_signs, out_signs, expert_ids, route_weight, cotangent,
              mean_weight, rho_weight, noise_weight):
    hidden_out, grad_tokens, grad_mean, grad_rho = layer(
        *(pltpu.with_memory_space_constraint(v, pltpu.HBM) for v in (
            tokens, in_signs.T, out_signs.T, expert_ids.T, route_weight.T, cotangent.T)),
        mean_weight[0], rho_weight[0], noise_weight[0])
    return hidden_out.T, grad_tokens, grad_mean[None], grad_rho[None]


def solution(mesh):
    row = P("expert", "dp")
    full = P("expert", None)
    weight = P("expert", "dp", None)
    return jax.shard_map(
        on_device, mesh=mesh,
        in_specs=(row, row, full, full, full, row, weight, weight, weight),
        out_specs=(row, row, weight, weight), check_vma=False)
```

```python
import jax
import jax.numpy as jnp
from jax import lax
from jax.experimental import pallas as pl
from jax.experimental.pallas import tpu as pltpu
from jax.sharding import PartitionSpec as P

F32 = jnp.float32
BF16 = jnp.bfloat16
I32 = jnp.int32
MESH = pl.DeviceIdType.MESH
NN = (((1,), (0,)), ((), ()))
TN = (((0,), (0,)), ((), ()))
VMEM = pl.BlockSpec(memory_space=pltpu.VMEM)

SIDE = 4
HALF = 112
OFFS = (2, 1, 3, 0)
CUT = ((0, 64), (64, 48))


NT = (((1,), (1,)), ((), ()))


def dot(a, b, dims=NN):
    return lax.dot_general(a, b, dims, preferred_element_type=F32)


VLIM = 50
ZORDER = (4, 3, 5, 2, 6, 1, 7)
UNITS = 7168
BLOCK = 896
COPIES = 35 + 1 + 16 + 24 + 6 + 2 + 2 + 8 + 8 + 16


def layer_kernel(tokens_hbm, ins_hbm, outs_hbm, ids_hbm, route_hbm, cot_hbm, mean_hbm, rho_hbm, noise_hbm,
                 hidden_out, grad_tokens, gm, gr,
                 tokens, in_signs, out_signs, ids, route, cotangent, picks, rows_in, words_in, cot_in, hid_out, back_out, mean, rho, noise, wm, wd, rows_r, words_r, words_p, cot_r, w2, bda, bdb, ba, bb, sgn_t,
                 up2, mx, dx, p, r0, q, t1, rp, rm, s, t2, rp2, rm2, dbuf, hs, dyr, accm, accd,
                 gt, gdt, gs, send, recv, local):
    me, z = lax.axis_index("dp"), lax.axis_index("expert")
    k = lax.rem(me, 2)
    x, y = me // 8, lax.rem(me // 2, SIDE)
    a, b = x * (1 - k) + y * k, y * (1 - k) + x * k
    sa, sb = 8 - 6 * k, 2 + 6 * k
    partner = me + 1 - 2 * k

    def at(da, db):
        return lax.rem(a + da, SIDE) * sa + lax.rem(b + db, SIDE) * sb + k

    def theirs(db, da):
        return lax.rem(b + db, SIDE) * sb + lax.rem(a + da, SIDE) * sa + (1 - k)

    up_a, down_a, up_b, down_b = at(1, 0), at(3, 0), at(0, 1), at(0, 3)

    loads = [pltpu.make_async_copy(src, dst, local.at[i]) for i, (src, dst) in enumerate(
        ((rho_hbm, rho), (noise_hbm, noise), (mean_hbm, mean), (ids_hbm, ids), (outs_hbm, out_signs),
         (ins_hbm, in_signs), (tokens_hbm, tokens), (route_hbm, route), (cot_hbm, cotangent)))]
    for c in loads[3:] + loads[:3]:
        c.start()
    barrier = pltpu.get_barrier_semaphore()
    for o in ZORDER:
        pl.semaphore_signal(barrier, inc=1, device_id={"expert": lax.rem(z + o, 8)}, device_id_type=MESH)
    for peer in (up_a, down_a, up_b, down_b, partner):
        pl.semaphore_signal(barrier, inc=1, device_id={"dp": peer}, device_id_type=MESH)

    for c in loads[3:]:
        c.wait()
    lane128 = lax.broadcasted_iota(I32, (128, 128), 1)
    row128 = lax.broadcasted_iota(I32, (128, 128), 0)
    names = [jnp.broadcast_to(ids[c:c + 1, :], (128, 128)) == row128 for c in range(2)]
    named = jnp.where(names[0] | names[1], 1.0, 0.0).astype(BF16)
    before = dot(named, jnp.where(row128 < lane128, 1.0, 0.0).astype(BF16))
    row320 = lax.broadcasted_iota(I32, (320, 128), 0)
    hit = []
    for c in range(2):
        rank = jnp.sum(jnp.where(names[c], before, 0.0), axis=0, keepdims=True).astype(I32)
        hit.append(jnp.broadcast_to(ids[c:c + 1, :] * 40 + rank, (320, 128)) == row320)
        picks[c] = jnp.where(hit[c], 1.0, 0.0).astype(BF16)
    gather_t = jnp.where(hit[0] | hit[1], 1.0, 0.0).astype(BF16)
    mine = jnp.where(k == 0, out_signs[0:112, :], out_signs[112:224, :])
    mine = jnp.concatenate([mine, in_signs[...], jnp.zeros((12, 128), I32)], axis=0)
    octets = jnp.concatenate(
        [((mine >> (8 * i)) & 255).astype(F32).astype(BF16) for i in range(4)], axis=0)
    octets = dot(gather_t, octets, NT).astype(I32)
    octets = (octets[:, 0:128] | (octets[:, 128:256] << 8)
              | (octets[:, 256:384] << 16) | (octets[:, 384:512] << 24))
    sent_rows = dot(gather_t, tokens[...])
    for e in range(8):
        words_in[e] = octets[40 * e:40 * e + 40]
        rows_in[e] = sent_rows[40 * e:40 * e + 40].astype(BF16)
    pl.semaphore_wait(barrier, 12)

    copies, done = [], set()

    def put(src, dst, to, axis="dp"):
        i = len(copies)
        c = pltpu.make_async_remote_copy(
            src, dst, send.at[i], recv.at[i], device_id={axis: to}, device_id_type=MESH)
        c.start()
        copies.append(c)
        return c

    def arrived(c):
        done.add(id(c))
        c.wait_recv()

    def swap(src, dst):
        out = []
        for o in ZORDER:
            to = lax.rem(z + o, 8)
            out.append(put(src.at[to], dst.at[z], to, "expert"))
        return out

    z_words = swap(words_in, words_r)
    z_rows = swap(rows_in, rows_r)
    weight_t = jnp.where(hit[0], route[0:1, :], 0.0) + jnp.where(hit[1], route[1:2, :], 0.0)
    sent_cot = dot(gather_t, cotangent[...], NT) * jnp.sum(weight_t, axis=1, keepdims=True)
    for e in range(8):
        cot_in[e] = sent_cot[40 * e:40 * e + 40].astype(BF16)
    z_cot = swap(cot_in, cot_r)
    words_r[z] = words_in[z]
    rows_r[z] = rows_in[z]
    cot_r[z] = cot_in[z]

    for c in loads[:3]:
        c.wait()

    def fold(i, carry):
        cols = pl.ds(pl.multiple_of(i * BLOCK, 128), BLOCK)
        delta = (jax.nn.softplus(rho[:, cols].astype(F32)) * noise[:, cols].astype(F32)).astype(BF16)
        for v, wt in ((mean[:, cols], wm), (delta, wd)):
            t = v.T
            for d in range(4):
                for h in range(2):
                    o = (2 * d + h) * HALF
                    wt[4 * i + d, :, h * 128:(h + 1) * 128] = t[o:o + HALF]
        return carry

    lax.fori_loop(0, 8, fold, 0)

    def slots_of(ref):
        return jnp.concatenate([ref[e].astype(F32) for e in range(8)], axis=0)

    for c in z_words:
        arrived(c)
    pair_words = put(words_r, words_p, partner)
    words = jnp.concatenate([words_r[e] for e in range(8)], axis=0)
    wt = words.T
    w2[k] = jnp.concatenate([wt, wt], axis=1)
    lane = lax.broadcasted_iota(I32, (320, 128), 1)
    word = jnp.broadcast_to(words[:, 115:116], (320, 128))
    for w in range(3):
        word = jnp.where(lane // 32 == w, jnp.broadcast_to(words[:, 112 + w:113 + w], (320, 128)), word)
    sgn = (1 - 2 * ((word >> (lane & 31)) & 1)).astype(F32)
    sgn_t[...] = sgn.T
    for c in z_rows:
        arrived(c)
    plain = slots_of(rows_r)
    signed = plain * sgn
    none_w = jnp.zeros((128, 320), F32)
    for v, wide in ((plain, bda), (signed, bdb)):
        t = v.T
        wide[0:128] = jnp.concatenate([t, none_w], axis=1).astype(BF16)
        wide[128:256] = jnp.concatenate([none_w, t], axis=1).astype(BF16)
    arrived(pair_words)
    wt = jnp.concatenate([words_p[e] for e in range(8)], axis=0).T
    w2[1 - k] = jnp.concatenate([wt, wt], axis=1)

    left = lax.broadcasted_iota(I32, (1, 640), 1) < 320
    down16 = lax.broadcasted_iota(I32, (16, 640), 0)

    def minus_at(dd, j):
        half, base = dd // 16, lax.rem(dd, 16) * 7
        one = w2[half, pl.ds(base + j // 2, 1), :] >> (16 * (j % 2))
        two = w2[half, pl.ds(base + 3 + (j + 1) // 2, 1), :] >> (16 * ((j + 1) % 2))
        return ((jnp.broadcast_to(jnp.where(left, one, two), (16, 640)) >> down16) & 1) != 0

    def products(dd_of):
        mx[...] = dot(jnp.concatenate([wm[dd_of(r)] for r in range(4)], axis=0), bda[...])
        dx[...] = dot(jnp.concatenate([wd[dd_of(r)] for r in range(4)], axis=0), bdb[...])

        for r in range(4):
            dd = dd_of(r)
            for j in range(7):
                o = r * HALF + 16 * j
                pert = dx[o:o + 16]
                p[dd, 16 * j:16 * j + 16] = (
                    mx[o:o + 16] + jnp.where(minus_at(dd, j), -pert, pert)).astype(BF16)

    pair = {}

    def products_pair(g):
        products(lambda r: theirs(OFFS[g], r))
        for r in range(4):
            pair[g, r] = put(p.at[theirs(OFFS[g], OFFS[r])], r0.at[4 * g + r], partner)

    def products_own(g):
        products(lambda r: at(OFFS[g], r))

    def merge(g, r):
        arrived(pair[g, r])
        q[4 * g + r] = p[at(OFFS[g], OFFS[r])] + r0[4 * g + r]

    far, plus, minus = {}, {}, {}
    (o0, n0), (o1, n1) = CUT
    c0, c1 = pl.ds(o0, n0), pl.ds(o1, n1)
    products_pair(0)
    products_own(0)
    products_pair(1)
    for r in range(4):
        merge(0, r)
        far[r] = (put(q.at[r, c0], t1.at[r, c0], up_a), put(q.at[r, c1], t1.at[r, c1], down_a))
    products_pair(2)
    products_own(1)
    products_own(2)
    products_pair(3)
    products_own(3)

    def relay(r):
        merge(1, r)
        plus[r] = [put(q.at[4 + r, c1], rp.at[r, c1], up_a)]
        merge(2, r)
        minus[r] = [put(q.at[8 + r, c0], rm.at[r, c0], down_a)]
        up, dn = far[r]
        arrived(up)
        q[4 + r, c0] = q[4 + r, c0] + t1[r, c0]
        plus[r].append(put(q.at[4 + r, c0], rp.at[r, c0], up_a))
        arrived(dn)
        q[8 + r, c1] = q[8 + r, c1] + t1[r, c1]
        minus[r].append(put(q.at[8 + r, c1], rm.at[r, c1], down_a))

    none_t = jnp.zeros((320, 128), F32)
    for v, tall in ((slots_of(rows_r), ba), (slots_of(rows_r) * sgn_t[...].T, bb)):
        tall[0:320] = jnp.concatenate([v, none_t], axis=1).astype(BF16)
        tall[320:640] = jnp.concatenate([none_t, v], axis=1).astype(BF16)
    for r in range(4):
        relay(r)
    for c in z_cot:
        arrived(c)
    ut = slots_of(cot_r).T
    up2[...] = jnp.concatenate([ut[:HALF], ut[HALF:]], axis=1)
    for r in range(4):
        merge(3, r)

    def total(r):
        for c in plus[r] + minus[r]:
            arrived(c)
        return q[12 + r].astype(F32) + rp[r].astype(F32) + rm[r].astype(F32)

    s[0] = total(0).astype(BF16)
    far_up = put(s.at[0, c0], t2.at[c0], up_b)
    far_dn = put(s.at[0, c1], t2.at[c1], down_b)
    s[1] = total(1).astype(BF16)
    p1 = put(s.at[1, c1], rp2.at[c1], up_b)
    s[2] = total(2).astype(BF16)
    m1 = put(s.at[2, c0], rm2.at[c0], down_b)
    arrived(far_up)
    s[1, c0] = s[1, c0] + t2[c0]
    p2 = put(s.at[1, c0], rp2.at[c0], up_b)
    arrived(far_dn)
    s[2, c1] = s[2, c1] + t2[c1]
    m2 = put(s.at[2, c1], rm2.at[c1], down_b)
    own = total(3)
    for c in (p1, m1, p2, m2):
        arrived(c)

    pre = own + rp2[...].astype(F32) + rm2[...].astype(F32)
    gate = jax.nn.sigmoid(pre)
    slope = gate * (1.0 + pre * (1.0 - gate))
    dbuf[me] = (up2[...] * slope).astype(BF16)

    def hand(da, db):
        i = at(da, db)
        hands[da, db] = put(dbuf.at[i], dbuf.at[i], partner)

    def spread(db):
        i = at(0, db)
        up = put(dbuf.at[i], dbuf.at[i], up_a)
        dn = put(dbuf.at[i], dbuf.at[i], down_a)
        hand(0, db)
        return up, dn

    hands = {}
    b_up = put(dbuf.at[me], dbuf.at[me], up_b)
    b_dn = put(dbuf.at[me], dbuf.at[me], down_b)
    sent = {0: spread(0)}

    ht = (pre * gate).T
    for e in range(8):
        hs[e] = jnp.concatenate(
            [ht[40 * e:40 * e + 40], ht[320 + 40 * e:360 + 40 * e]], axis=0).astype(BF16)
    z_hid = swap(hs, hid_out)
    hid_out[z] = hs[z]

    arrived(b_up)
    i = at(0, 3)
    f_up = put(dbuf.at[i, c0], dbuf.at[i, c0], up_b)
    arrived(b_dn)
    i = at(0, 1)
    f_dn = put(dbuf.at[i, c1], dbuf.at[i, c1], down_b)
    sent[3] = spread(3)
    sent[1] = spread(1)
    fwd = {}

    def arrive(db):
        up, dn = sent[db]
        arrived(up)
        i = at(3, db)
        fwd[db] = [put(dbuf.at[i, c0], dbuf.at[i, c0], up_a)]
        hand(3, db)
        arrived(dn)
        i = at(1, db)
        fwd[db].append(put(dbuf.at[i, c1], dbuf.at[i, c1], down_a))
        hand(1, db)

    def last(db):
        for c in fwd[db]:
            arrived(c)
        hand(2, db)

    def gradients(dd_of, first=False, keep_for=0):
        for r in range(4):
            dd = dd_of(r)
            for j in range(7):
                o = r * HALF + 16 * j
                v = dbuf[dd, 16 * j:16 * j + 16].astype(F32)
                dyr[keep_for, o:o + 16] = jnp.where(minus_at(dd, j), -v, v).astype(BF16)
        dds = [dd_of(r) for r in range(4)]
        dy = jnp.concatenate([dbuf[dd] for dd in dds], axis=0)
        gmean = dot(jnp.concatenate([wm[dd] for dd in dds], axis=0), dy, TN)
        gpert = dot(jnp.concatenate([wd[dd] for dd in dds], axis=0), dyr[keep_for], TN)
        if first:
            accm[...] = gmean
            accd[...] = gpert
        else:
            accm[...] += gmean
            accd[...] += gpert
        later = lambda: weights(dd_of, keep_for)
        if keep_for:
            return later
        later()

    def weights(dd_of, kept):
        dy = jnp.concatenate([dbuf[dd_of(r)] for r in range(4)], axis=0)
        mx[:, 0:256] = dot(dy, ba[...])
        mx[:, 256:512] = dot(dyr[kept], bb[...])

        def keep(r, carry):
            dd = dd_of(r)
            rows = pl.ds(pl.multiple_of(r * HALF, 16), HALF)
            for h in range(2):
                gt[2 * dd + h] = mx[rows, h * 128:(h + 1) * 128].astype(BF16)
                gdt[2 * dd + h] = mx[rows, 256 + h * 128:384 + h * 128]
            return carry

        lax.fori_loop(0, 4, keep, 0)

    def gradients_own(da, first=False, keep_for=0):
        return gradients(lambda r: at(da, r), first, keep_for)

    def gradients_pair(db, keep_for=0):
        for da in range(4):
            arrived(hands[db, da])
        return gradients(lambda r: theirs(db, r), False, keep_for)

    arrived(f_up)
    arrived(f_dn)
    sent[2] = spread(2)
    arrive(0)
    gradients_own(0, True)
    arrive(3)
    arrive(1)
    gradients_pair(0)
    arrive(2)
    gradients_own(3)
    last(0)
    gradients_own(1)
    last(3)
    last(1)
    gradients_pair(3)
    last(2)
    kept = [gradients_pair(1, 1), gradients_own(2, False, 2), gradients_pair(2, 3)]

    gp = accm[0:128, 0:320] + accm[128:256, 320:640]
    gn = accd[0:128, 0:320] + accd[128:256, 320:640]
    g = (gp + sgn_t[...] * gn).T
    for e in range(8):
        gs[e] = g[40 * e:40 * e + 40].astype(BF16)
    z_back = swap(gs, back_out)
    back_out[z] = gs[z]
    for rest in kept:
        rest()

    def turn(i, carry):
        cols = pl.ds(pl.multiple_of(i * BLOCK, 128), BLOCK)
        rows = pl.ds(8 * i, 8)
        gm[0, :, cols] = gt[rows].reshape(BLOCK, 128).T
        gr[0, :, cols] = (gdt[rows].reshape(BLOCK, 128).T * noise[:, cols].astype(F32)
                       * jax.nn.sigmoid(rho[:, cols].astype(F32))).astype(BF16)
        return carry

    lax.fori_loop(0, 8, turn, 0)
    for c in z_hid:
        arrived(c)
    for h in range(2):
        v = jnp.concatenate(
            [hid_out[e].astype(F32)[40 * h:40 * h + 40] for e in range(8)], axis=0).astype(BF16)
        hidden_out[HALF * h:HALF * h + HALF] = (
            dot(v, picks[0], TN) * route[0:1, :] + dot(v, picks[1], TN) * route[1:2, :]).astype(BF16)
    for c in z_back:
        arrived(c)
    grad_tokens[...] = dot(picks[0] + picks[1], slots_of(back_out).astype(BF16), TN).astype(BF16)

    for c in copies:
        if id(c) not in done:
            c.wait_recv()
    for c in copies:
        c.wait_send()
    assert len(copies) == COPIES


def layer(*args):
    v = pltpu.VMEM
    blk = lambda n: v((n, HALF, 640), BF16)
    one = v((HALF, 640), BF16)
    weight = v((128, UNITS), BF16)
    hbm = pl.BlockSpec(memory_space=pltpu.HBM)
    return pl.pallas_call(
        layer_kernel,
        in_specs=[hbm] * 9,
        out_specs=[VMEM] * 4,
        out_shape=[jax.ShapeDtypeStruct((224, 128), BF16), jax.ShapeDtypeStruct((128, 128), BF16),
                   jax.ShapeDtypeStruct((1, 128, UNITS), BF16), jax.ShapeDtypeStruct((1, 128, UNITS), BF16)],
        scratch_shapes=[
            v((128, 128), BF16), v((4, 128), I32), v((224, 128), I32), v((2, 128), I32), v((2, 128), F32),
            v((224, 128), BF16), v((2, 320, 128), BF16), v((8, 40, 128), BF16), v((8, 40, 128), I32), v((8, 40, 224), BF16),
            v((8, 80, HALF), BF16), v((8, 40, 128), BF16),
            weight, weight, weight, v((32, HALF, 256), BF16), v((32, HALF, 256), BF16),
            v((8, 40, 128), BF16), v((8, 40, 128), I32), v((8, 40, 128), I32), v((8, 40, 224), BF16),
            v((2, 128, 640), I32), v((256, 640), BF16), v((256, 640), BF16),
            v((640, 256), BF16), v((640, 256), BF16), v((128, 320), F32), v((HALF, 640), F32),
            v((448, 640), F32), v((448, 640), F32),
            blk(32), blk(16), blk(16), blk(4), blk(4), blk(4), blk(3), one, one, one, blk(32),
            v((8, 80, HALF), BF16), v((4, 448, 640), BF16), v((256, 640), F32), v((256, 640), F32),
            v((64, HALF, 128), BF16), v((64, HALF, 128), F32), v((8, 40, 128), BF16),
            pltpu.SemaphoreType.DMA((COPIES,)), pltpu.SemaphoreType.DMA((COPIES,)),
            pltpu.SemaphoreType.DMA((9,))],
        compiler_params=pltpu.CompilerParams(
            collective_id=1, has_side_effects=True, vmem_limit_bytes=VLIM * 1024 * 1024),
        name="layer",
    )(*args)


def out_kernel(hid, tok, gm, gr, hid_hbm, tok_hbm, gm_hbm, gr_hbm, sem):
    parts = [(hid, hid_hbm), (tok, tok_hbm)]
    for ref, hbm in ((gm, gm_hbm), (gr, gr_hbm)):
        parts += [(ref.at[0, pl.ds(32 * i, 32)], hbm.at[0, pl.ds(32 * i, 32)]) for i in range(4)]
    copies = [pltpu.make_async_copy(src, dst, sem.at[i]) for i, (src, dst) in enumerate(parts)]
    for c in copies:
        c.start()
    for c in copies:
        c.wait()


def out(*arrays):
    hbm = pl.BlockSpec(memory_space=pl.ANY)
    return pl.pallas_call(
        out_kernel,
        in_specs=[VMEM] * 4,
        out_specs=[hbm] * 4,
        out_shape=[jax.ShapeDtypeStruct(v.shape, v.dtype) for v in arrays],
        scratch_shapes=[pltpu.SemaphoreType.DMA((10,))],
        compiler_params=pltpu.CompilerParams(vmem_limit_bytes=8 * 1024 * 1024),
        name="out",
    )(*arrays)


def on_device(tokens, in_signs, out_signs, expert_ids, route_weight, cotangent,
              mean_weight, rho_weight, noise_weight):
    hidden_out, grad_tokens, grad_mean, grad_rho = out(*layer(
        *(pltpu.with_memory_space_constraint(v, pltpu.HBM) for v in (
            tokens, in_signs.T, out_signs.T, expert_ids.T, route_weight.T, cotangent.T)),
        mean_weight[0], rho_weight[0], noise_weight[0]))
    return hidden_out.T, grad_tokens, grad_mean, grad_rho


def solution(mesh):
    row = P("expert", "dp")
    full = P("expert", None)
    weight = P("expert", "dp", None)
    return jax.shard_map(
        on_device, mesh=mesh,
        in_specs=(row, row, full, full, full, row, weight, weight, weight),
        out_specs=(row, row, weight, weight), check_vma=False)
```

```python
import jax
import jax.numpy as jnp
from jax import lax
from jax.experimental import pallas as pl
from jax.experimental.pallas import tpu as pltpu
from jax.sharding import PartitionSpec as P

F32 = jnp.float32
BF16 = jnp.bfloat16
I32 = jnp.int32
MESH = pl.DeviceIdType.MESH
NN = (((1,), (0,)), ((), ()))
TN = (((0,), (0,)), ((), ()))
VMEM = pl.BlockSpec(memory_space=pltpu.VMEM)

SIDE = 4
HALF = 112
OFFS = (2, 1, 3, 0)
CUT = ((0, 64), (64, 48))


NT = (((1,), (1,)), ((), ()))


def dot(a, b, dims=NN):
    return lax.dot_general(a, b, dims, preferred_element_type=F32)


VLIM = 50
ZORDER = (4, 3, 5, 2, 6, 1, 7)
UNITS = 7168
BLOCK = 896
COPIES = 35 + 1 + 16 + 24 + 6 + 2 + 2 + 8 + 8 + 16


def layer_kernel(tokens_hbm, ins_hbm, outs_hbm, ids_hbm, route_hbm, cot_hbm, mean_hbm, rho_hbm, noise_hbm,
                 hidden_out, grad_tokens, gm, gr,
                 tokens, in_signs, out_signs, ids, route, cotangent, picks, rows_in, words_in, cot_in, hid_out, back_out, mean, rho, noise, wm, wd, rows_r, words_r, words_p, cot_r, w2, bda, bdb, ba, bb, sgn_t,
                 up2, mx, dx, p, r0, q, t1, rp, rm, s, t2, rp2, rm2, dbuf, hs, dyr, accm, accd,
                 gt, gdt, gs, send, recv, local):
    me, z = lax.axis_index("dp"), lax.axis_index("expert")
    k = lax.rem(me, 2)
    x, y = me // 8, lax.rem(me // 2, SIDE)
    a, b = x * (1 - k) + y * k, y * (1 - k) + x * k
    sa, sb = 8 - 6 * k, 2 + 6 * k
    partner = me + 1 - 2 * k

    def at(da, db):
        return lax.rem(a + da, SIDE) * sa + lax.rem(b + db, SIDE) * sb + k

    def theirs(db, da):
        return lax.rem(b + db, SIDE) * sb + lax.rem(a + da, SIDE) * sa + (1 - k)

    up_a, down_a, up_b, down_b = at(1, 0), at(3, 0), at(0, 1), at(0, 3)

    loads = [pltpu.make_async_copy(src, dst, local.at[i]) for i, (src, dst) in enumerate(
        ((rho_hbm, rho), (noise_hbm, noise), (mean_hbm, mean), (ids_hbm, ids), (outs_hbm, out_signs),
         (ins_hbm, in_signs), (tokens_hbm, tokens), (route_hbm, route), (cot_hbm, cotangent)))]
    for c in loads[3:] + loads[:3]:
        c.start()
    barrier = pltpu.get_barrier_semaphore()
    for o in ZORDER:
        pl.semaphore_signal(barrier, inc=1, device_id={"expert": lax.rem(z + o, 8)}, device_id_type=MESH)
    for peer in (up_a, down_a, up_b, down_b, partner):
        pl.semaphore_signal(barrier, inc=1, device_id={"dp": peer}, device_id_type=MESH)

    for c in loads[3:]:
        c.wait()
    lane128 = lax.broadcasted_iota(I32, (128, 128), 1)
    row128 = lax.broadcasted_iota(I32, (128, 128), 0)
    names = [jnp.broadcast_to(ids[c:c + 1, :], (128, 128)) == row128 for c in range(2)]
    named = jnp.where(names[0] | names[1], 1.0, 0.0).astype(BF16)
    before = dot(named, jnp.where(row128 < lane128, 1.0, 0.0).astype(BF16))
    row320 = lax.broadcasted_iota(I32, (320, 128), 0)
    hit = []
    for c in range(2):
        rank = jnp.sum(jnp.where(names[c], before, 0.0), axis=0, keepdims=True).astype(I32)
        hit.append(jnp.broadcast_to(ids[c:c + 1, :] * 40 + rank, (320, 128)) == row320)
        picks[c] = jnp.where(hit[c], 1.0, 0.0).astype(BF16)
    gather_t = jnp.where(hit[0] | hit[1], 1.0, 0.0).astype(BF16)
    mine = jnp.where(k == 0, out_signs[0:112, :], out_signs[112:224, :])
    mine = jnp.concatenate([mine, in_signs[...], jnp.zeros((12, 128), I32)], axis=0)
    octets = jnp.concatenate(
        [((mine >> (8 * i)) & 255).astype(F32).astype(BF16) for i in range(4)], axis=0)
    octets = dot(gather_t, octets, NT).astype(I32)
    octets = (octets[:, 0:128] | (octets[:, 128:256] << 8)
              | (octets[:, 256:384] << 16) | (octets[:, 384:512] << 24))
    sent_rows = dot(gather_t, tokens[...])
    for e in range(8):
        words_in[e] = octets[40 * e:40 * e + 40]
        rows_in[e] = sent_rows[40 * e:40 * e + 40].astype(BF16)
    pl.semaphore_wait(barrier, 12)

    copies, done = [], set()

    def put(src, dst, to, axis="dp"):
        i = len(copies)
        c = pltpu.make_async_remote_copy(
            src, dst, send.at[i], recv.at[i], device_id={axis: to}, device_id_type=MESH)
        c.start()
        copies.append(c)
        return c

    def arrived(c):
        done.add(id(c))
        c.wait_recv()

    def swap(src, dst):
        out = []
        for o in ZORDER:
            to = lax.rem(z + o, 8)
            out.append(put(src.at[to], dst.at[z], to, "expert"))
        return out

    z_words = swap(words_in, words_r)
    z_rows = swap(rows_in, rows_r)
    weight_t = jnp.where(hit[0], route[0:1, :], 0.0) + jnp.where(hit[1], route[1:2, :], 0.0)
    sent_cot = dot(gather_t, cotangent[...], NT) * jnp.sum(weight_t, axis=1, keepdims=True)
    for e in range(8):
        cot_in[e] = sent_cot[40 * e:40 * e + 40].astype(BF16)
    z_cot = swap(cot_in, cot_r)
    words_r[z] = words_in[z]
    rows_r[z] = rows_in[z]
    cot_r[z] = cot_in[z]

    for c in loads[:3]:
        c.wait()

    def fold(i, carry):
        cols = pl.ds(pl.multiple_of(i * BLOCK, 128), BLOCK)
        delta = (jax.nn.softplus(rho[:, cols].astype(F32)) * noise[:, cols].astype(F32)).astype(BF16)
        for v, wt in ((mean[:, cols], wm), (delta, wd)):
            t = v.T
            for d in range(4):
                for h in range(2):
                    o = (2 * d + h) * HALF
                    wt[4 * i + d, :, h * 128:(h + 1) * 128] = t[o:o + HALF]
        return carry

    lax.fori_loop(0, 8, fold, 0)

    def slots_of(ref):
        return jnp.concatenate([ref[e].astype(F32) for e in range(8)], axis=0)

    for c in z_words:
        arrived(c)
    pair_words = put(words_r, words_p, partner)
    words = jnp.concatenate([words_r[e] for e in range(8)], axis=0)
    wt = words.T
    w2[k] = jnp.concatenate([wt, wt], axis=1)
    lane = lax.broadcasted_iota(I32, (320, 128), 1)
    word = jnp.broadcast_to(words[:, 115:116], (320, 128))
    for w in range(3):
        word = jnp.where(lane // 32 == w, jnp.broadcast_to(words[:, 112 + w:113 + w], (320, 128)), word)
    sgn = (1 - 2 * ((word >> (lane & 31)) & 1)).astype(F32)
    sgn_t[...] = sgn.T
    for c in z_rows:
        arrived(c)
    plain = slots_of(rows_r)
    signed = plain * sgn
    none_w = jnp.zeros((128, 320), F32)
    for v, wide in ((plain, bda), (signed, bdb)):
        t = v.T
        wide[0:128] = jnp.concatenate([t, none_w], axis=1).astype(BF16)
        wide[128:256] = jnp.concatenate([none_w, t], axis=1).astype(BF16)
    arrived(pair_words)
    wt = jnp.concatenate([words_p[e] for e in range(8)], axis=0).T
    w2[1 - k] = jnp.concatenate([wt, wt], axis=1)

    left = lax.broadcasted_iota(I32, (1, 640), 1) < 320
    down16 = lax.broadcasted_iota(I32, (16, 640), 0)

    def minus_at(dd, j):
        half, base = dd // 16, lax.rem(dd, 16) * 7
        one = w2[half, pl.ds(base + j // 2, 1), :] >> (16 * (j % 2))
        two = w2[half, pl.ds(base + 3 + (j + 1) // 2, 1), :] >> (16 * ((j + 1) % 2))
        return ((jnp.broadcast_to(jnp.where(left, one, two), (16, 640)) >> down16) & 1) != 0

    def products(dd_of):
        mx[...] = dot(jnp.concatenate([wm[dd_of(r)] for r in range(4)], axis=0), bda[...])
        dx[...] = dot(jnp.concatenate([wd[dd_of(r)] for r in range(4)], axis=0), bdb[...])

        for r in range(4):
            dd = dd_of(r)
            for j in range(7):
                o = r * HALF + 16 * j
                pert = dx[o:o + 16]
                p[dd, 16 * j:16 * j + 16] = (
                    mx[o:o + 16] + jnp.where(minus_at(dd, j), -pert, pert)).astype(BF16)

    pair = {}

    def products_pair(g):
        products(lambda r: theirs(OFFS[g], r))
        for r in range(4):
            pair[g, r] = put(p.at[theirs(OFFS[g], OFFS[r])], r0.at[4 * g + r], partner)

    def products_own(g):
        products(lambda r: at(OFFS[g], r))

    def merge(g, r):
        arrived(pair[g, r])
        q[4 * g + r] = p[at(OFFS[g], OFFS[r])] + r0[4 * g + r]

    far, plus, minus = {}, {}, {}
    (o0, n0), (o1, n1) = CUT
    c0, c1 = pl.ds(o0, n0), pl.ds(o1, n1)
    products_pair(0)
    products_own(0)
    products_pair(1)
    def start(r):
        merge(0, r)
        far[r] = (put(q.at[r, c0], t1.at[r, c0], up_a), put(q.at[r, c1], t1.at[r, c1], down_a))

    for r in range(3):
        start(r)
    products_pair(2)
    products_own(1)
    products_own(2)

    def plain_rows(r):
        merge(1, r)
        plus[r] = [put(q.at[4 + r, c1], rp.at[r, c1], up_a)]
        merge(2, r)
        minus[r] = [put(q.at[8 + r, c0], rm.at[r, c0], down_a)]

    def added_rows(r):
        up, dn = far[r]
        arrived(up)
        q[4 + r, c0] = q[4 + r, c0] + t1[r, c0]
        plus[r].append(put(q.at[4 + r, c0], rp.at[r, c0], up_a))
        arrived(dn)
        q[8 + r, c1] = q[8 + r, c1] + t1[r, c1]
        minus[r].append(put(q.at[8 + r, c1], rm.at[r, c1], down_a))

    def relay(r):
        plain_rows(r)
        added_rows(r)

    relay(0)
    products_pair(3)
    products_own(3)
    none_t = jnp.zeros((320, 128), F32)
    for v, tall in ((slots_of(rows_r), ba), (slots_of(rows_r) * sgn_t[...].T, bb)):
        tall[0:320] = jnp.concatenate([v, none_t], axis=1).astype(BF16)
        tall[320:640] = jnp.concatenate([none_t, v], axis=1).astype(BF16)
    relay(1)
    relay(2)
    start(3)
    plain_rows(3)
    for c in z_cot:
        arrived(c)
    ut = slots_of(cot_r).T
    up2[...] = jnp.concatenate([ut[:HALF], ut[HALF:]], axis=1)
    for r in range(4):
        merge(3, r)

    def total(r):
        for c in plus[r] + minus[r]:
            arrived(c)
        return q[12 + r].astype(F32) + rp[r].astype(F32) + rm[r].astype(F32)

    s[0] = total(0).astype(BF16)
    far_up = put(s.at[0, c0], t2.at[c0], up_b)
    far_dn = put(s.at[0, c1], t2.at[c1], down_b)
    s[1] = total(1).astype(BF16)
    p1 = put(s.at[1, c1], rp2.at[c1], up_b)
    s[2] = total(2).astype(BF16)
    m1 = put(s.at[2, c0], rm2.at[c0], down_b)
    arrived(far_up)
    s[1, c0] = s[1, c0] + t2[c0]
    p2 = put(s.at[1, c0], rp2.at[c0], up_b)
    arrived(far_dn)
    s[2, c1] = s[2, c1] + t2[c1]
    m2 = put(s.at[2, c1], rm2.at[c1], down_b)
    added_rows(3)
    own = total(3)
    for c in (p1, m1, p2, m2):
        arrived(c)

    pre = own + rp2[...].astype(F32) + rm2[...].astype(F32)
    gate = jax.nn.sigmoid(pre)
    slope = gate * (1.0 + pre * (1.0 - gate))
    dbuf[me] = (up2[...] * slope).astype(BF16)

    def hand(da, db):
        i = at(da, db)
        hands[da, db] = put(dbuf.at[i], dbuf.at[i], partner)

    def spread(db):
        i = at(0, db)
        up = put(dbuf.at[i], dbuf.at[i], up_a)
        dn = put(dbuf.at[i], dbuf.at[i], down_a)
        hand(0, db)
        return up, dn

    hands = {}
    b_up = put(dbuf.at[me], dbuf.at[me], up_b)
    b_dn = put(dbuf.at[me], dbuf.at[me], down_b)
    sent = {0: spread(0)}

    ht = (pre * gate).T
    for e in range(8):
        hs[e] = jnp.concatenate(
            [ht[40 * e:40 * e + 40], ht[320 + 40 * e:360 + 40 * e]], axis=0).astype(BF16)
    z_hid = swap(hs, hid_out)
    hid_out[z] = hs[z]

    arrived(b_up)
    i = at(0, 3)
    f_up = put(dbuf.at[i, c0], dbuf.at[i, c0], up_b)
    arrived(b_dn)
    i = at(0, 1)
    f_dn = put(dbuf.at[i, c1], dbuf.at[i, c1], down_b)
    sent[3] = spread(3)
    sent[1] = spread(1)
    fwd = {}

    def arrive(db):
        up, dn = sent[db]
        arrived(up)
        i = at(3, db)
        fwd[db] = [put(dbuf.at[i, c0], dbuf.at[i, c0], up_a)]
        hand(3, db)
        arrived(dn)
        i = at(1, db)
        fwd[db].append(put(dbuf.at[i, c1], dbuf.at[i, c1], down_a))
        hand(1, db)

    def last(db):
        for c in fwd[db]:
            arrived(c)
        hand(2, db)

    def gradients(dd_of, first=False, keep_for=0):
        for r in range(4):
            dd = dd_of(r)
            for j in range(7):
                o = r * HALF + 16 * j
                v = dbuf[dd, 16 * j:16 * j + 16].astype(F32)
                dyr[keep_for, o:o + 16] = jnp.where(minus_at(dd, j), -v, v).astype(BF16)
        dds = [dd_of(r) for r in range(4)]
        dy = jnp.concatenate([dbuf[dd] for dd in dds], axis=0)
        gmean = dot(jnp.concatenate([wm[dd] for dd in dds], axis=0), dy, TN)
        gpert = dot(jnp.concatenate([wd[dd] for dd in dds], axis=0), dyr[keep_for], TN)
        if first:
            accm[...] = gmean
            accd[...] = gpert
        else:
            accm[...] += gmean
            accd[...] += gpert
        later = lambda: weights(dd_of, keep_for)
        if keep_for:
            return later
        later()

    def weights(dd_of, kept):
        dy = jnp.concatenate([dbuf[dd_of(r)] for r in range(4)], axis=0)
        mx[:, 0:256] = dot(dy, ba[...])
        mx[:, 256:512] = dot(dyr[kept], bb[...])

        def keep(r, carry):
            dd = dd_of(r)
            rows = pl.ds(pl.multiple_of(r * HALF, 16), HALF)
            for h in range(2):
                gt[2 * dd + h] = mx[rows, h * 128:(h + 1) * 128].astype(BF16)
                gdt[2 * dd + h] = mx[rows, 256 + h * 128:384 + h * 128]
            return carry

        lax.fori_loop(0, 4, keep, 0)

    def gradients_own(da, first=False, keep_for=0):
        return gradients(lambda r: at(da, r), first, keep_for)

    def gradients_pair(db, keep_for=0):
        for da in range(4):
            arrived(hands[db, da])
        return gradients(lambda r: theirs(db, r), False, keep_for)

    arrived(f_up)
    arrived(f_dn)
    sent[2] = spread(2)
    arrive(0)
    gradients_own(0, True)
    arrive(3)
    arrive(1)
    gradients_pair(0)
    arrive(2)
    gradients_own(3)
    last(0)
    gradients_own(1)
    last(3)
    last(1)
    gradients_pair(3)
    last(2)
    kept = [gradients_pair(1, 1), gradients_own(2, False, 2), gradients_pair(2, 3)]

    gp = accm[0:128, 0:320] + accm[128:256, 320:640]
    gn = accd[0:128, 0:320] + accd[128:256, 320:640]
    g = (gp + sgn_t[...] * gn).T
    for e in range(8):
        gs[e] = g[40 * e:40 * e + 40].astype(BF16)
    z_back = swap(gs, back_out)
    back_out[z] = gs[z]
    for rest in kept:
        rest()

    def turn(i, carry):
        cols = pl.ds(pl.multiple_of(i * BLOCK, 128), BLOCK)
        rows = pl.ds(8 * i, 8)
        gm[0, :, cols] = gt[rows].reshape(BLOCK, 128).T
        gr[0, :, cols] = (gdt[rows].reshape(BLOCK, 128).T * noise[:, cols].astype(F32)
                       * jax.nn.sigmoid(rho[:, cols].astype(F32))).astype(BF16)
        return carry

    lax.fori_loop(0, 8, turn, 0)
    for c in z_hid:
        arrived(c)
    for h in range(2):
        v = jnp.concatenate(
            [hid_out[e].astype(F32)[40 * h:40 * h + 40] for e in range(8)], axis=0).astype(BF16)
        hidden_out[HALF * h:HALF * h + HALF] = (
            dot(v, picks[0], TN) * route[0:1, :] + dot(v, picks[1], TN) * route[1:2, :]).astype(BF16)
    for c in z_back:
        arrived(c)
    grad_tokens[...] = dot(picks[0] + picks[1], slots_of(back_out).astype(BF16), TN).astype(BF16)

    for c in copies:
        if id(c) not in done:
            c.wait_recv()
    for c in copies:
        c.wait_send()
    assert len(copies) == COPIES


def layer(*args):
    v = pltpu.VMEM
    blk = lambda n: v((n, HALF, 640), BF16)
    one = v((HALF, 640), BF16)
    weight = v((128, UNITS), BF16)
    hbm = pl.BlockSpec(memory_space=pltpu.HBM)
    return pl.pallas_call(
        layer_kernel,
        in_specs=[hbm] * 9,
        out_specs=[VMEM] * 4,
        out_shape=[jax.ShapeDtypeStruct((224, 128), BF16), jax.ShapeDtypeStruct((128, 128), BF16),
                   jax.ShapeDtypeStruct((1, 128, UNITS), BF16), jax.ShapeDtypeStruct((1, 128, UNITS), BF16)],
        scratch_shapes=[
            v((128, 128), BF16), v((4, 128), I32), v((224, 128), I32), v((2, 128), I32), v((2, 128), F32),
            v((224, 128), BF16), v((2, 320, 128), BF16), v((8, 40, 128), BF16), v((8, 40, 128), I32), v((8, 40, 224), BF16),
            v((8, 80, HALF), BF16), v((8, 40, 128), BF16),
            weight, weight, weight, v((32, HALF, 256), BF16), v((32, HALF, 256), BF16),
            v((8, 40, 128), BF16), v((8, 40, 128), I32), v((8, 40, 128), I32), v((8, 40, 224), BF16),
            v((2, 128, 640), I32), v((256, 640), BF16), v((256, 640), BF16),
            v((640, 256), BF16), v((640, 256), BF16), v((128, 320), F32), v((HALF, 640), F32),
            v((448, 640), F32), v((448, 640), F32),
            blk(32), blk(16), blk(16), blk(4), blk(4), blk(4), blk(3), one, one, one, blk(32),
            v((8, 80, HALF), BF16), v((4, 448, 640), BF16), v((256, 640), F32), v((256, 640), F32),
            v((64, HALF, 128), BF16), v((64, HALF, 128), F32), v((8, 40, 128), BF16),
            pltpu.SemaphoreType.DMA((COPIES,)), pltpu.SemaphoreType.DMA((COPIES,)),
            pltpu.SemaphoreType.DMA((9,))],
        compiler_params=pltpu.CompilerParams(
            collective_id=1, has_side_effects=True, vmem_limit_bytes=VLIM * 1024 * 1024),
        name="layer",
    )(*args)


def out_kernel(hid, tok, gm, gr, hid_hbm, tok_hbm, gm_hbm, gr_hbm, sem):
    parts = [(hid, hid_hbm), (tok, tok_hbm)]
    for ref, hbm in ((gm, gm_hbm), (gr, gr_hbm)):
        parts += [(ref.at[0, pl.ds(32 * i, 32)], hbm.at[0, pl.ds(32 * i, 32)]) for i in range(4)]
    copies = [pltpu.make_async_copy(src, dst, sem.at[i]) for i, (src, dst) in enumerate(parts)]
    for c in copies:
        c.start()
    for c in copies:
        c.wait()


def out(*arrays):
    hbm = pl.BlockSpec(memory_space=pl.ANY)
    return pl.pallas_call(
        out_kernel,
        in_specs=[VMEM] * 4,
        out_specs=[hbm] * 4,
        out_shape=[jax.ShapeDtypeStruct(v.shape, v.dtype) for v in arrays],
        scratch_shapes=[pltpu.SemaphoreType.DMA((10,))],
        compiler_params=pltpu.CompilerParams(vmem_limit_bytes=8 * 1024 * 1024),
        name="out",
    )(*arrays)


def on_device(tokens, in_signs, out_signs, expert_ids, route_weight, cotangent,
              mean_weight, rho_weight, noise_weight):
    hidden_out, grad_tokens, grad_mean, grad_rho = out(*layer(
        *(pltpu.with_memory_space_constraint(v, pltpu.HBM) for v in (
            tokens, in_signs.T, out_signs.T, expert_ids.T, route_weight.T, cotangent.T)),
        mean_weight[0], rho_weight[0], noise_weight[0]))
    return hidden_out.T, grad_tokens, grad_mean, grad_rho


def solution(mesh):
    row = P("expert", "dp")
    full = P("expert", None)
    weight = P("expert", "dp", None)
    return jax.shard_map(
        on_device, mesh=mesh,
        in_specs=(row, row, full, full, full, row, weight, weight, weight),
        out_specs=(row, row, weight, weight), check_vma=False)
```
